32 devices in a mesh: curve: 32 (over z, y, x, core).
Axes of the slice: x: 2, y: 2, z: 4, core: 2. Of those that a mesh axis runs over, the one named last changes fastest.
Arguments:
- nodal_state: float32 [5, 64, 16384], P(None, None, 'curve'), may hold values from -9 to 9, as said below
- inverse_jacobian: float32 [16384], P('curve'), may hold values from 1 to 4
- speeds: float32 [3, 5], replicated, may hold values from -1.5 to 1.5
- refine_flags: int32 [16384], P('curve'), may hold values from 0 to 1, as said below
- send_index: int32 [12288], P('curve'), may hold values from 0 to 3071, as said below
- face_source: int32 [6, 16384], P(None, 'curve'), may hold values from 0 to 3455, as said below
Outputs:
- refined_state: float32 [5, 64, 30720], P(None, None, 'curve')
- refined_jacobian: float32 [30720], P('curve')
The draws below stay inside these ranges and needn't reach their ends.
Inputs may be any that keep to these rules, and one draw needn't show every extreme that they name: `nodal_state`: each element's 64 node values are a level plus a linear part plus noise of an amplitude that varies from element to element. `refine_flags`: exactly 64 flags per device on average over all devices, at most 128 on one device, a number that is reached; the refined elements of a device go only to itself and its two curve neighbours, at most 224 to each neighbour, a number that is reached. `send_index`: per device, four blocks of 96 entries for destination offsets -2, -1, 1, 2 along the curve (cyclically): entries f * 512 + n of the traces that device reads, in increasing order, then zeros in unused slots; the blocks for offsets -1 and 1 are always full. `face_source`: face pairing is symmetric: across face 2 d of an element lies face 2 d + 1 of its neighbour; neighbours are on the same device or on one within two curve offsets.
All inputs are finite; a program needn't handle non-finite values.
Results may differ from the reference program's by a relative error of at most 0.0003.
Values sent between devices are 32-bit elements; how exact they have to be, the bound alone decides.
No kernel may reach another device: no remote copies, remote signals or barrier semaphores. Data moves between devices by JAX's collectives and lax.ppermute only.
A program may use at most 64 MiB of HBM per device.

```python
import math
import jax
import jax.numpy as jnp
import numpy as np
from jax import lax

VARS = 5
E_DEV = 512
FLAG_DEV = 64
HALO_W = 16
HALO_SLOTS = 96
ELEMS = 16384
NEW_ELEMS = 30720
N_CURVE = 32


def random_orders(key, count_rows, length):
    return jax.vmap(lambda single: jax.random.permutation(single, length))(jax.random.split(key, count_rows)).astype(jnp.int32)


def band_offsets(key, length, band_width):
    far_counts = jax.random.randint(key, (2,), 1, band_width + 1).astype(jnp.int32)
    edge_one = far_counts[0]
    edge_two = edge_one + band_width
    edge_three = edge_two + band_width
    edge_four = edge_three + far_counts[1]
    ranks = jnp.arange(length, dtype=jnp.int32)
    return jnp.where(ranks < edge_one, -2, jnp.where(ranks < edge_two, -1, jnp.where(ranks < edge_three, 1, jnp.where(ranks < edge_four, 2, 0)))).astype(jnp.int32)


def offset_slot(offset):
    return jnp.where(offset < 0, offset + 2, offset + 1).astype(jnp.int32)


def forest_tables(key):
    devices = N_CURVE
    elements = E_DEV
    slot_count = HALO_SLOTS
    base_key = jax.random.fold_in(key, 11)
    device_ids = jnp.arange(devices, dtype=jnp.int32)[:, None]
    neighbours = []
    for direction in range(3):
        dir_key = jax.random.fold_in(base_key, direction)
        first_key, second_key, band_key = jax.random.split(dir_key, 3)
        first = random_orders(first_key, devices, elements)
        second = random_orders(second_key, devices, elements)
        first_inverse = jnp.argsort(first, axis=1).astype(jnp.int32)
        second_inverse = jnp.argsort(second, axis=1).astype(jnp.int32)
        bands = band_offsets(band_key, elements, HALO_W)
        ahead = bands[first]
        target = (device_ids + ahead) % devices
        forward = target * elements + second[target, first]
        behind = bands[second_inverse]
        anchor = (device_ids - behind) % devices
        backward = anchor * elements + first_inverse[anchor, second_inverse]
        neighbours.append(forward)
        neighbours.append(backward)
    near_ids = jnp.stack(neighbours).astype(jnp.int32)
    owner = near_ids // elements
    relative = (owner - device_ids[None] + 2) % devices - 2
    slot_of = jnp.where(relative == 0, 4, offset_slot(relative)).astype(jnp.int32)
    flat_slot = jnp.transpose(slot_of, (1, 0, 2)).reshape(devices, 6 * elements)
    flat_ids = jnp.arange(6 * elements, dtype=jnp.int32)[None, :]
    sort_keys = flat_slot * (6 * elements) + flat_ids
    ordering = jnp.argsort(sort_keys, axis=1).astype(jnp.int32)
    position = jnp.argsort(ordering, axis=1).astype(jnp.int32)
    starts = jnp.stack([jnp.sum(flat_slot < block, axis=1) for block in range(4)], axis=1).astype(jnp.int32)
    counts = jnp.stack([jnp.sum(flat_slot == block, axis=1) for block in range(4)], axis=1).astype(jnp.int32)
    lanes = jnp.arange(slot_count, dtype=jnp.int32)
    picks = jnp.minimum(starts[:, :, None] + lanes[None, None, :], 6 * elements - 1)
    sent = jnp.take_along_axis(ordering, picks.reshape(devices, 4 * slot_count), axis=1).reshape(devices, 4, slot_count)
    sent = jnp.where(lanes[None, None, :] < counts[:, :, None], sent, 0).astype(jnp.int32)
    faces = jnp.arange(6, dtype=jnp.int32)[:, None, None]
    partner = faces + 1 - 2 * (faces % 2)
    sender_flat = partner * elements + near_ids % elements
    rank_at = position[owner, sender_flat] - starts[owner, offset_slot(-relative)]
    ghost_index = 6 * elements + offset_slot(relative) * slot_count + rank_at
    source = jnp.where(relative == 0, sender_flat, ghost_index).astype(jnp.int32)
    return (sent.reshape(-1), source.reshape(6, devices * elements))


def draw_send_index(key, part):
    return forest_tables(key)[0]


def draw_face_source(key, part):
    return forest_tables(key)[1]


def draw_refine_flags(key, part):
    devices = N_CURVE
    elements = E_DEV
    half_flags = FLAG_DEV // 2
    drift_key, spot_key, order_key = jax.random.split(jax.random.fold_in(key, 5), 3)
    drift_by = jax.random.randint(drift_key, (devices,), -half_flags, half_flags + 1).astype(jnp.int32)
    spot_at = jax.random.randint(spot_key, (), 1, devices - 1).astype(jnp.int32)
    device_ids = jnp.arange(devices, dtype=jnp.int32)
    drift_by = jnp.where(device_ids == spot_at - 1, -half_flags, drift_by)
    drift_by = jnp.where(device_ids == spot_at, half_flags, drift_by)
    drift_by = jnp.where(device_ids == devices - 1, 0, drift_by).astype(jnp.int32)
    before = jnp.concatenate([jnp.zeros((1,), jnp.int32), drift_by[:-1]])
    counts = FLAG_DEV + drift_by - before
    orders = random_orders(order_key, devices, elements)
    return (orders < counts[:, None]).astype(jnp.int32).reshape(-1)


def draw_nodal_state(key, part):
    first_key, second_key, third_key, fourth_key = jax.random.split(jax.random.fold_in(key, 3), 4)
    element_total = ELEMS
    root = 1.0 / math.sqrt(5.0)
    points = jnp.array([-1.0, -root, root, 1.0], jnp.float32)
    node_ids = jnp.arange(64, dtype=jnp.int32)
    node_positions = jnp.stack([points[node_ids % 4], points[node_ids // 4 % 4], points[node_ids // 16]])
    level = 0.6 * jax.random.truncated_normal(first_key, -3.0, 3.0, (5, 1, element_total), jnp.float32)
    gradient_slopes = 0.4 * jax.random.truncated_normal(second_key, -3.0, 3.0, (5, 3, element_total), jnp.float32)
    incline_factor = jnp.einsum('whz,hq->wqz', gradient_slopes, node_positions)
    rough = jnp.exp(jax.random.uniform(third_key, (1, 1, element_total), jnp.float32, math.log(0.03), 0.0))
    noise = jax.random.truncated_normal(fourth_key, -3.0, 3.0, (5, 64, element_total), jnp.float32)
    return (level + incline_factor + rough * noise).astype(jnp.float32)


def level_of(rng, shape, cuts, smallest, top_value):
    def one(dim, parts):
        draws = jax.random.uniform(jax.random.fold_in(jax.random.fold_in(rng, 6), dim), (parts,), jnp.float32, smallest / len(cuts), top_value / len(cuts))
        return jnp.repeat(jnp.exp(draws), shape[dim] // parts).reshape((-1,) + (1,) * (len(shape) - dim - 1))

    level = one(*cuts[0])
    for cut in cuts[1:]:
        level = level * one(*cut)
    return level


def setup_inputs(seed: int = 0) -> dict:
    streams_of = jax.random.split(jax.random.key(seed), 7)
    return {
        "nodal_state": draw_nodal_state(jax.random.fold_in(streams_of[6], 71), 0),
        "inverse_jacobian": jnp.clip(jnp.exp(math.log(4.0) - 1.3862944 * jax.random.uniform(streams_of[1], (ELEMS,), jnp.float32) ** level_of(streams_of[1], (ELEMS,), ((0, 32),), -0.2, 0.2)), 1.0, 4.0),
        "speeds": jnp.clip(jax.random.uniform(streams_of[2], (3, VARS), jnp.float32, -1.5, 1.5), -1.5, 1.5),
        "refine_flags": draw_refine_flags(jax.random.fold_in(streams_of[6], 71), 0),
        "send_index": draw_send_index(jax.random.fold_in(streams_of[6], 71), 0),
        "face_source": draw_face_source(jax.random.fold_in(streams_of[6], 71), 0),
    }


time_step = 0.02

def lagrange_at(points, targets):
    values_at = np.ones((len(targets), 4))
    for basis_id in range(4):
        for partner in range(4):
            if partner != basis_id:
                values_at[:, basis_id] *= (targets - points[partner]) / (points[basis_id] - points[partner])
    return values_at

def modes_table(points):
    mono_to_legendre = np.array([[1.0, 0.0, 0.0, 0.0], [0.0, 1.0, 0.0, 0.0], [1.0 / 3.0, 0.0, 2.0 / 3.0, 0.0], [0.0, 0.6, 0.0, 0.4]])
    table = np.zeros((4, 4))
    for basis_id in range(4):
        coef = [1.0, 0.0, 0.0, 0.0]
        for partner in range(4):
            if partner != basis_id:
                denom = points[basis_id] - points[partner]
                fresh = [0.0, 0.0, 0.0, 0.0]
                for power in range(4):
                    lower = coef[power - 1] if power > 0 else 0.0
                    fresh[power] = (lower - points[partner] * coef[power]) / denom
                coef = fresh
        legendre = np.zeros(4)
        for power in range(4):
            legendre = legendre + coef[power] * mono_to_legendre[power]
        table[:, basis_id] = legendre
    return table

def node_constants():
    root = 1.0 / math.sqrt(5.0)
    points = np.array([-1.0, -root, root, 1.0])
    weights = np.array([1.0, 5.0, 5.0, 1.0]) / 6.0
    barycentric = np.ones(4)
    for node_row in range(4):
        for node_col in range(4):
            if node_row != node_col:
                barycentric[node_row] /= points[node_row] - points[node_col]
    deriv = np.zeros((4, 4))
    for node_row in range(4):
        for node_col in range(4):
            if node_row != node_col:
                deriv[node_row, node_col] = barycentric[node_col] / barycentric[node_row] / (points[node_row] - points[node_col])
        deriv[node_row, node_row] = -np.sum(deriv[node_row])
    to_modes = modes_table(points)
    sides = [lagrange_at(points, (points - 1.0) / 2.0), lagrange_at(points, (points + 1.0) / 2.0)]
    prolong = np.stack([np.kron(sides[child_id >> 2 & 1], np.kron(sides[child_id >> 1 & 1], sides[child_id & 1])) for child_id in range(8)])
    degrees = np.arange(4)
    levels = np.maximum(np.maximum(degrees[:, None, None], degrees[None, :, None]), degrees[None, None, :])
    top_mask = np.where(levels == 3, 1.0, 0.0)
    return (jnp.asarray(deriv, jnp.float32), jnp.asarray(weights, jnp.float32), jnp.asarray(to_modes, jnp.float32), jnp.asarray(prolong, jnp.float32), jnp.asarray(top_mask, jnp.float32))

def apply_along(matrix, values, node_axis):
    forms = {1: 'ak,vkjie->vajie', 2: 'aj,vkjie->vkaie', 3: 'ai,vkjie->vkjae'}
    return jnp.einsum(forms[node_axis], matrix, values, precision=lax.Precision.HIGHEST)

def face_flux(left_side, right_side, speed_dim):
    central = speed_dim * (left_side * left_side + left_side * right_side + right_side * right_side) / 6.0
    reach_by = jnp.abs(speed_dim) * jnp.maximum(jnp.abs(left_side), jnp.abs(right_side))
    return central - 0.5 * reach_by * (right_side - left_side)

def face_traces(shaped):
    element_count = shaped.shape[4]
    layers = []
    for dim_id in range(3):
        node_axis = 3 - dim_id
        for side_at in (0, 3):
            layers.append(lax.slice_in_dim(shaped, side_at, side_at + 1, axis=node_axis).reshape(5, 16, element_count))
    return jnp.stack(layers, axis=2)

def section_update(shaped, outside, speeds, inverse_jacobian):
    deriv, weights, to_modes, prolong, top_mask = node_constants()
    modal_coef = apply_along(to_modes, apply_along(to_modes, apply_along(to_modes, shaped[0:1], 1), 2), 3)[0]
    energy = modal_coef * modal_coef
    high_part = lax.optimization_barrier(jnp.sum(energy * top_mask[:, :, :, None], axis=(0, 1, 2)))
    all_part = lax.optimization_barrier(jnp.sum(energy, axis=(0, 1, 2)))
    top_ratio = high_part / (all_part + 1e-06)
    blend_weight = 0.5 * top_ratio / (top_ratio + 0.1)
    high_rate = jnp.zeros_like(shaped)
    lower_order_rate = jnp.zeros_like(shaped)
    for dim_id in range(3):
        node_axis = 3 - dim_id
        shape_w = [1, 1, 1, 1, 1]
        shape_w[node_axis] = 4
        node_weights = weights.reshape(shape_w)
        speed_dim = speeds[dim_id].reshape(5, 1, 1, 1, 1)
        volume = -(speed_dim / 3.0) * (shaped * apply_along(deriv, shaped, node_axis) + apply_along(deriv, shaped * shaped, node_axis))
        first_layer = lax.slice_in_dim(shaped, 0, 1, axis=node_axis)
        last_layer = lax.slice_in_dim(shaped, 3, 4, axis=node_axis)
        outer_left = outside[:, :, 2 * dim_id, :].reshape(first_layer.shape)
        outer_right = outside[:, :, 2 * dim_id + 1, :].reshape(first_layer.shape)
        flux_left = face_flux(outer_left, first_layer, speed_dim)
        flux_right = face_flux(last_layer, outer_right, speed_dim)
        middle = jnp.zeros_like(lax.slice_in_dim(shaped, 1, 3, axis=node_axis))
        surface_terms = jnp.concatenate([6.0 * (flux_left - 0.5 * speed_dim * first_layer * first_layer), middle, -6.0 * (flux_right - 0.5 * speed_dim * last_layer * last_layer)], axis=node_axis)
        inner_flux = face_flux(lax.slice_in_dim(shaped, 0, 3, axis=node_axis), lax.slice_in_dim(shaped, 1, 4, axis=node_axis), speed_dim)
        fluxes = jnp.concatenate([flux_left, inner_flux, flux_right], axis=node_axis)
        low_dim = -(lax.slice_in_dim(fluxes, 1, 5, axis=node_axis) - lax.slice_in_dim(fluxes, 0, 4, axis=node_axis)) / node_weights
        high_rate = high_rate + volume + surface_terms
        lower_order_rate = lower_order_rate + low_dim
    rate_all = inverse_jacobian * ((1.0 - blend_weight) * high_rate + blend_weight * lower_order_rate)
    return shaped + time_step * rate_all

def refine_block(updated, jacobian, flag_ids, flag_most):
    deriv, weights, to_modes, prolong, top_mask = node_constants()
    element_count = updated.shape[2]
    capacity = element_count + 7 * flag_most
    flag_ids = flag_ids.astype(jnp.int32)
    before = jnp.cumsum(flag_ids).astype(jnp.int32) - flag_ids
    element_ids = jnp.arange(element_count, dtype=jnp.int32)
    slot_ids = jnp.where(flag_ids == 1, before, flag_most).astype(jnp.int32)
    listing = jnp.zeros((flag_most,), jnp.int32).at[slot_ids].set(element_ids, mode='drop')
    chosen = jnp.take(updated, listing, axis=2)
    stacked = jnp.transpose(chosen, (1, 0, 2)).reshape(64, 5 * flag_most)
    children = jnp.dot(prolong.reshape(512, 64), stacked, precision=lax.Precision.HIGHEST, preferred_element_type=jnp.float32)
    children = jnp.transpose(children.reshape(8, 64, 5, flag_most), (2, 1, 0, 3)).reshape(5, 64, 8 * flag_most)
    placed = element_ids + 7 * before
    updated_refine_marks = jnp.zeros((capacity,), jnp.int32).at[placed].add(1)
    parent = jnp.clip(jnp.cumsum(updated_refine_marks).astype(jnp.int32) - 1, 0, element_count - 1)
    new_ids = jnp.arange(capacity, dtype=jnp.int32)
    child_id = new_ids - placed[parent]
    parent_flag = flag_ids[parent]
    new_total = (element_count + 7 * jnp.sum(flag_ids)).astype(jnp.int32)
    source = jnp.where(parent_flag == 1, element_count + child_id * flag_most + before[parent], parent)
    source = jnp.where(new_ids < new_total, source, 0).astype(jnp.int32)
    refined = jnp.take(jnp.concatenate([updated, children], axis=2), source, axis=2)
    new_jac = jacobian[parent] * jnp.where(parent_flag == 1, 2.0, 1.0).astype(jacobian.dtype)
    return (refined, new_jac, new_total)

def reference(nodal_state, inverse_jacobian, speeds, refine_flags, send_index, face_source):
    devices = N_CURVE
    elements = E_DEV
    slot_count = HALO_SLOTS
    element_total = devices * elements
    shaped = nodal_state.reshape(5, 4, 4, 4, element_total)
    traces = face_traces(shaped)
    trace_table = jnp.transpose(traces.reshape(5, 16, 6, devices, elements), (0, 1, 3, 2, 4)).reshape(5, 16, devices * 6 * elements)
    receiver = (jnp.arange(element_total, dtype=jnp.int32) // elements)[None, :]
    ghost_id = face_source - 6 * elements
    place_id = jnp.clip(ghost_id // slot_count, 0, 3)
    lane_id = jnp.clip(ghost_id - place_id * slot_count, 0, slot_count - 1)
    shifts = jnp.array([-2, -1, 1, 2], jnp.int32)
    sender = (receiver + shifts[place_id]) % devices
    blocks = send_index.reshape(devices, 4, slot_count)
    sent_flat = blocks[sender, 3 - place_id, lane_id]
    global_ids = jnp.where(face_source < 6 * elements, receiver * 6 * elements + face_source, sender * 6 * elements + sent_flat).astype(jnp.int32)
    outside = jnp.take(trace_table, global_ids.reshape(-1), axis=2).reshape(5, 16, 6, element_total)
    updated = section_update(shaped, outside, speeds, inverse_jacobian).reshape(5, 64, element_total)
    refined, new_jac, new_total = refine_block(updated, inverse_jacobian, refine_flags, FLAG_DEV * devices)
    return (refined[:, :, :NEW_ELEMS], new_jac[:NEW_ELEMS])
```

```python
import math

import jax
import jax.numpy as jnp
import numpy as np
from jax import lax
from jax.experimental import pallas as pl
from jax.experimental.pallas import tpu as pltpu
from jax.sharding import PartitionSpec as P

E_NEW = 960
TIME_STEP = 0.02
OFFSETS = (-2, -1, 1, 2)
LANES = 128
BF = jnp.bfloat16
F32 = jnp.float32


def lagrange_at(points, targets):
    values_at = np.ones((len(targets), 4))
    for basis_id in range(4):
        for partner in range(4):
            if partner != basis_id:
                values_at[:, basis_id] *= (targets - points[partner]) / (
                    points[basis_id] - points[partner]
                )
    return values_at


def modes_table(points):
    return np.linalg.inv(np.polynomial.legendre.legvander(points, 3))


def node_constants():
    root = 1.0 / math.sqrt(5.0)
    points = np.array([-1.0, -root, root, 1.0])
    deriv = np.zeros((4, 4))
    bary = np.array([1.0 / np.prod([points[r] - points[c] for c in range(4) if c != r]) for r in range(4)])
    for r in range(4):
        for c in range(4):
            if r != c:
                deriv[r, c] = bary[c] / bary[r] / (points[r] - points[c])
        deriv[r, r] = -np.sum(deriv[r])
    sides = (lagrange_at(points, (points - 1.0) / 2.0), lagrange_at(points, (points + 1.0) / 2.0))
    return deriv, modes_table(points), sides


DERIV, MODES, SIDES = node_constants()
INV_W = (6.0, 1.2, 1.2, 6.0)
SELF_SURFACE = (-3.0, 0.0, 0.0, 3.0)


def low_half(shape=(8, LANES)):
    return lax.broadcasted_iota(jnp.int32, shape, 0) < 4


def swap_halves(x):
    return pltpu.roll(x, 4, axis=0)


def trace_of(ref, t, face):
    dim, side = face // 2, face % 2
    if dim == 0:
        return ref[t, pl.ds(3 * side, 16, stride=4), :]
    if dim == 2:
        return ref[t, 48 * side : 48 * side + 16, :]
    low = low_half()
    tiles = [ref[t, 16 * k + 8 * side : 16 * k + 8 * side + 8, :] for k in range(4)]
    halves = []
    for k in (0, 2):
        if side == 0:
            halves.append(jnp.where(low, tiles[k], swap_halves(tiles[k + 1])))
        else:
            halves.append(jnp.where(low, swap_halves(tiles[k]), tiles[k + 1]))
    return jnp.concatenate(halves, axis=0)


def add_to_face(ref, t, face, value):
    dim, side = face // 2, face % 2
    if dim == 0:
        where_at = (t, pl.ds(3 * side, 16, stride=4), slice(None))
        ref[where_at] = ref[where_at] + value
    elif dim == 2:
        where_at = (t, slice(48 * side, 48 * side + 16), slice(None))
        ref[where_at] = ref[where_at] + value
    else:
        low = low_half()
        keep = low if side == 0 else jnp.logical_not(low)
        for k in range(4):
            half = value[8 * (k // 2) : 8 * (k // 2) + 8, :]
            if (k % 2) != side:
                half = swap_halves(half)
            where_at = (t, slice(16 * k + 8 * side, 16 * k + 8 * side + 8), slice(None))
            ref[where_at] = ref[where_at] + jnp.where(keep, half, 0.0)


def split_two(x):
    high = x.astype(BF)
    return high, (x - high.astype(F32)).astype(BF)


def one_hot(row, count):
    ids = lax.broadcasted_iota(jnp.int32, (count, row.shape[1]), 0)
    return jnp.where(ids == row, 1.0, 0.0).astype(BF)


def dot32(a, b):
    return jnp.dot(a, b, preferred_element_type=F32)


def send_kernel(u_ref, idx_ref, jac_ref, flag_ref, *rest):
    outs, lhs, gathered = rest[:4], rest[4], rest[5]
    elements = u_ref.shape[2]
    slots = idx_ref.shape[1] // 4
    for v in range(5):
        high, low = split_two(u_ref[v])
        lhs[v * 64 : (v + 1) * 64, :] = high
        lhs[320 + v * 64 : 320 + (v + 1) * 64, :] = low
    row = jnp.broadcast_to(idx_ref[...], (8, 4 * slots))
    row = jnp.concatenate([row, jnp.zeros((8, 512 - 4 * slots), jnp.int32)], axis=1)
    blocks = [row[:, :LANES]]
    for b in range(1, 4):
        blocks.append(pltpu.roll(row, 512 - slots * b, axis=1)[:, :LANES])
    idx = jnp.concatenate(blocks, axis=1)
    face = jnp.zeros_like(idx)
    for f in range(1, 6):
        face = face + (idx >= f * elements).astype(jnp.int32)
    elem = idx - face * elements
    picked = dot32(lhs[...], one_hot(elem[0:1], elements))
    for b in range(4):
        part = picked[:320, b * LANES : (b + 1) * LANES] + picked[320:, b * LANES : (b + 1) * LANES]
        gathered[b * 5 : (b + 1) * 5] = part.reshape(5, 64, LANES)
    flags = flag_ref[...].astype(F32)
    count = elements + 7.0 * jnp.sum(flags)
    rows = lax.broadcasted_iota(jnp.int32, (8, LANES), 0)
    groups = elements // LANES
    for b in range(4):
        fb = jnp.broadcast_to(face[0:1, b * LANES : (b + 1) * LANES], (16, LANES))
        for v in range(5):
            value = trace_of(gathered, b * 5 + v, 0)
            for f in range(1, 6):
                value = jnp.where(fb == f, trace_of(gathered, b * 5 + v, f), value)
            outs[b][v * 16 : (v + 1) * 16, :] = value
        near = 0 if OFFSETS[b] < 0 else groups - 2
        meta = jnp.full((8, LANES), count, F32)
        for r in range(2):
            meta = jnp.where(rows == r, jac_ref[near + r : near + r + 1, :], meta)
            meta = jnp.where(rows == 2 + r, flags[near + r : near + r + 1, :], meta)
        outs[b][80:88, :] = meta


def line_rates(x, speed, blend):
    square = [x[m] * x[m] for m in range(4)]
    prod = {}
    for m in range(4):
        for n in range(m + 1, 4):
            prod[m, n] = x[m] * x[n]
    half_speed = 0.5 * jnp.abs(speed)
    flux = []
    for m in range(3):
        central = square[m] + prod[m, m + 1] + square[m + 1]
        reach = jnp.maximum(jnp.abs(x[m]), jnp.abs(x[m + 1]))
        flux.append((speed / 6.0) * central - half_speed * reach * (x[m + 1] - x[m]))
    out = []
    for n in range(4):
        high = None
        diag = -2.0 * DERIV[n, n] / 3.0 + SELF_SURFACE[n]
        for m in range(4):
            if m != n:
                pair = prod[min(m, n), max(m, n)] + square[m]
                term = float(-DERIV[n, m] / 3.0) * pair
                high = term if high is None else high + term
        if n in (0, 3):
            high = high + float(diag) * square[n]
        high = speed * high
        if n == 0:
            low = -INV_W[0] * flux[0]
        elif n == 3:
            low = INV_W[3] * flux[2]
        else:
            low = INV_W[n] * (flux[n - 1] - flux[n])
        out.append(high + blend * (low - high))
    return out


def local_kernel(u_ref, jac_ref, fs_ref, sp_ref, modes_ref, base_ref, slab_ref, out_ref, lhs, rows_s):
    elements = u_ref.shape[2]
    groups = elements // LANES
    for v in range(5):
        for g in range(groups):
            slab_ref[g * 5 + v] = u_ref[v, :, g * LANES : (g + 1) * LANES]
    modal = jnp.dot(
        modes_ref[:, :64], u_ref[0], precision=lax.Precision.HIGHEST, preferred_element_type=F32
    )
    energy = modal * modal
    top = jnp.sum(energy * modes_ref[:, 64:65], axis=0, keepdims=True)
    whole = jnp.sum(energy, axis=0, keepdims=True)
    ratio = top / (whole + 1e-06)
    blend_all = 0.5 * ratio / (ratio + 0.1)
    for g in range(groups):
        rows_s[g] = jnp.broadcast_to(blend_all[:, g * LANES : (g + 1) * LANES], (8, LANES))
        rows_s[groups + g] = jnp.broadcast_to(jac_ref[g : g + 1, :] * TIME_STEP, (8, LANES))

    def one(t, carry):
        g = t // 5
        v = t - 5 * g
        blend = rows_s[g]
        scale = rows_s[groups + g]
        low = low_half()
        for kh in range(2):
            at = [(t, pl.ds(32 * kh + i, 8, stride=4), slice(None)) for i in range(4)]
            rate = line_rates([slab_ref[a] for a in at], sp_ref[0, v], blend)
            for i in range(4):
                base_ref[at[i]] = rate[i]
        tile = [[slab_ref[t, 16 * k + 8 * h : 16 * k + 8 * h + 8, :] for h in range(2)] for k in range(4)]
        rates = [[None, None] for _ in range(4)]
        for h in range(2):
            r = line_rates([tile[k][h] for k in range(4)], sp_ref[2, v], blend)
            for k in range(4):
                rates[k][h] = r[k]
        for k in (0, 2):
            x = []
            for h in range(2):
                x.append(jnp.where(low, tile[k][h], swap_halves(tile[k + 1][h])))
                x.append(jnp.where(low, swap_halves(tile[k][h]), tile[k + 1][h]))
            r = line_rates(x, sp_ref[1, v], blend)
            for h in range(2):
                first, second = r[2 * h], r[2 * h + 1]
                rates[k][h] = rates[k][h] + jnp.where(low, first, swap_halves(second))
                rates[k + 1][h] = rates[k + 1][h] + jnp.where(low, swap_halves(first), second)
        for k in range(4):
            for h in range(2):
                at = (t, slice(16 * k + 8 * h, 16 * k + 8 * h + 8), slice(None))
                base_ref[at] = tile[k][h] + scale * (rates[k][h] + base_ref[at])
        return carry

    lax.fori_loop(0, 5 * groups, one, 0)

    for f in range(6):
        partner = f + 1 - 2 * (f % 2)
        for g in range(groups):
            for v in range(5):
                high, low = split_two(trace_of(slab_ref, g * 5 + v, partner))
                lhs[v * 16 : (v + 1) * 16, g * LANES : (g + 1) * LANES] = high
                lhs[80 + v * 16 : 80 + (v + 1) * 16, g * LANES : (g + 1) * LANES] = low
        picked = dot32(lhs[...], one_hot(fs_ref[f : f + 1, :] - partner * elements, elements))
        near = fs_ref[f : f + 1, :] < 6 * elements
        out_ref[f] = jnp.where(near, picked[:80] + picked[80:], 0.0)


def face_kernel(base_ref, slab_ref, out_ref, fs_ref, jac_ref, sp_ref, flag_ref, r0, r1, r2, r3, *rest):
    head_ref, tail_ref, width_ref, lhs, outside = rest
    elements = fs_ref.shape[1]
    groups = elements // LANES
    slots = 96
    for b, ref in enumerate((r0, r1, r2, r3)):
        high, low = split_two(ref[0:80, :])
        lhs[0:80, b * LANES : (b + 1) * LANES] = high
        lhs[80:160, b * LANES : (b + 1) * LANES] = low
    half = 5 * (groups // 2)
    head_ref[...] = base_ref[0:half]
    tail_ref[...] = base_ref[half : 2 * half]
    for f in range(6):
        ghost = fs_ref[f : f + 1, :] - 6 * elements
        place = jnp.zeros_like(ghost)
        for b in range(1, 4):
            place = place + (ghost >= b * slots).astype(jnp.int32)
        column = ghost + place * (LANES - slots)
        picked = dot32(lhs[...], one_hot(column, 4 * LANES))
        outside[f] = out_ref[f] + (picked[:80] + picked[80:])
    for g in range(groups):
        ref, first = (head_ref, 0) if g < groups // 2 else (tail_ref, groups // 2)
        scale = jnp.broadcast_to(jac_ref[g : g + 1, :] * TIME_STEP, (16, LANES))
        for v in range(5):
            t = g * 5 + v
            for f in range(6):
                speed = sp_ref[f // 2, v]
                inner = trace_of(slab_ref, t, f)
                outer = outside[f, v * 16 : (v + 1) * 16, g * LANES : (g + 1) * LANES]
                central = inner * inner + inner * outer + outer * outer
                reach = (3.0 * jnp.abs(speed)) * jnp.maximum(jnp.abs(inner), jnp.abs(outer))
                sign = 1.0 if f % 2 == 0 else -1.0
                value = (sign * speed) * central - reach * (inner - outer)
                add_to_face(ref, (g - first) * 5 + v, f, scale * value)
    me = lax.axis_index("curve")
    total = lax.axis_size("curve")
    lower = me < total // 2
    count = jnp.full((8, LANES), elements + 7.0 * jnp.sum(flag_ref[...].astype(F32)), F32)
    own = count
    for o, ref in zip(OFFSETS, (r0, r1, r2, r3)):
        there = me + o
        wanted = jnp.logical_and(lower if o < 0 else jnp.logical_not(lower), jnp.logical_and(there >= 0, there < total))
        value = jnp.broadcast_to(ref[87:88, :], (8, LANES))
        count = count + value * jnp.where(wanted, 1.0, 0.0)
    width_ref[0:8] = count
    width_ref[8:16] = own


def refine_kernel(low_ref, head_ref, tail_ref, up_ref, w_ref, own_ref, r1, r2, jac_ref, flag_ref, *rest):
    out_ref, jout_ref, lhs, res, coef, cols = rest
    halves = (low_ref, head_ref, tail_ref, up_ref)
    total = lax.axis_size("curve")
    me = lax.axis_index("curve")
    for b, ref in enumerate(halves):
        for g in range(2):
            high, low = split_two(ref[5 * g : 5 * g + 5].reshape(320, LANES))
            at = slice((2 * b + g) * LANES, (2 * b + g + 1) * LANES)
            lhs[0:320, at] = high
            lhs[320:640, at] = low
    jac = jnp.concatenate([r1[80:82, :], jac_ref[...], r2[80:82, :]], axis=0)
    flag = jnp.concatenate([r1[82:84, :], flag_ref[...].astype(F32), r2[82:84, :]], axis=0)
    sizes = 1.0 + 7.0 * flag
    lane0 = lax.broadcasted_iota(jnp.int32, (LANES, LANES), 0)
    lane1 = lax.broadcasted_iota(jnp.int32, (LANES, LANES), 1)
    upper = jnp.where(lane0 < lane1, 1.0, 0.0).astype(BF)
    sizes_b = sizes.astype(BF)
    within = dot32(sizes_b, upper)
    row_total = jnp.sum(sizes, axis=1, keepdims=True)
    running = jnp.zeros((1, 1), F32)
    starts = []
    for r in range(8):
        starts.append(running)
        running = running + row_total[r : r + 1]
    row0 = lax.broadcasted_iota(jnp.int32, (8, LANES), 0)
    before = within
    for r in range(8):
        before = before + jnp.where(row0 == r, starts[r], 0.0)
    width = w_ref[0:8]
    if own_ref is not None:
        width = width
    mine = own_ref[8:16]
    lower = jnp.where(me < total // 2, 1.0, 0.0)
    begin = lower * (width - mine) + (1.0 - lower) * (float(total * E_NEW) - width)
    begin = begin - (me * E_NEW).astype(F32)
    place = before + (begin - starts[2])
    ends = place + sizes
    place_hi = jnp.floor(place * (1.0 / 256.0))
    place_lo = place - 256.0 * place_hi
    jac_a = jac.astype(BF)
    jac_b = (jac - jac_a.astype(F32)).astype(BF)
    jac_c = (jac - jac_a.astype(F32) - jac_b.astype(F32)).astype(BF)
    rows16 = lax.broadcasted_iota(jnp.int32, (16, LANES), 0)
    extras = [jac_a.astype(F32), jac_b.astype(F32), jac_c.astype(F32), flag, place_hi, place_lo]
    for r in range(8):
        block = jnp.zeros((16, LANES), F32)
        for q, item in enumerate(extras):
            block = jnp.where(rows16 == q, jnp.broadcast_to(item[r : r + 1, :], (16, LANES)), block)
        lhs[640:656, r * LANES : (r + 1) * LANES] = block.astype(BF)
        cols[0, r * LANES : (r + 1) * LANES, :] = jnp.transpose(jnp.broadcast_to(place[r : r + 1, :], (LANES, LANES)))
        cols[1, r * LANES : (r + 1) * LANES, :] = jnp.transpose(jnp.broadcast_to(ends[r : r + 1, :], (LANES, LANES)))

    spans = ((0, 768), (256, 768), (256, 1024), (256, 1024))
    for pair, (k0, k1) in enumerate(spans):
        pieces = []
        for h in range(2):
            slot = (lax.broadcasted_iota(jnp.int32, (8, LANES), 1) + (2 * pair + h) * LANES).astype(F32)
            slot_b = jnp.broadcast_to(slot[0:1], (k1 - k0, LANES))
            hit = jnp.logical_and(slot_b >= cols[0, k0:k1, :], slot_b < cols[1, k0:k1, :])
            pieces.append(jnp.where(hit, 1.0, 0.0).astype(BF))
        picked = dot32(lhs[:, k0:k1], jnp.concatenate(pieces, axis=1))
        for h in range(2):
            g = 2 * pair + h
            lanes = slice(h * LANES, (h + 1) * LANES)
            width_at = min(LANES, E_NEW - g * LANES)
            res[...] = (picked[0:320, lanes] + picked[320:640, lanes]).reshape(5, 64, LANES)
            extra = picked[640:656, lanes]
            jac_new = (extra[0:1] + extra[1:2] + extra[2:3]) * (1.0 + extra[3:4])
            jout_ref[0:1, g * LANES : g * LANES + width_at] = jac_new[:, :width_at]
            fl = jnp.broadcast_to(extra[3:4], (8, LANES))
            slot = (lax.broadcasted_iota(jnp.int32, (8, LANES), 1) + g * LANES).astype(F32)
            child = slot - (256.0 * extra[4:5] + extra[5:6])
            bit2 = jnp.where(child >= 4.0, 1.0, 0.0)
            child = child - 4.0 * bit2
            bit1 = jnp.where(child >= 2.0, 1.0, 0.0)
            bit0 = child - 2.0 * bit1
            for d, bit in enumerate((bit0, bit1, bit2)):
                both = fl * bit
                for i in range(4):
                    for m in range(4):
                        eye = 1.0 if i == m else 0.0
                        c = fl * float(SIDES[0][i, m] - eye) + both * float(SIDES[1][i, m] - SIDES[0][i, m]) + eye
                        coef[16 * d + 4 * i + m] = c

            def apply(d, x):
                out = []
                for i in range(4):
                    acc = coef[16 * d + 4 * i] * x[0]
                    for m in range(1, 4):
                        acc = acc + coef[16 * d + 4 * i + m] * x[m]
                    out.append(acc)
                return out

            def one(v, carry):
                low = low_half()
                for kh in range(2):
                    at = [(v, pl.ds(32 * kh + i, 8, stride=4), slice(None)) for i in range(4)]
                    y = apply(0, [res[a] for a in at])
                    for i in range(4):
                        res[at[i]] = y[i]
                tile = [[res[v, 16 * k + 8 * q : 16 * k + 8 * q + 8, :] for q in range(2)] for k in range(4)]
                for q in range(2):
                    y = apply(2, [tile[k][q] for k in range(4)])
                    for k in range(4):
                        tile[k][q] = y[k]
                for k in (0, 2):
                    x = []
                    for q in range(2):
                        x.append(jnp.where(low, tile[k][q], swap_halves(tile[k + 1][q])))
                        x.append(jnp.where(low, swap_halves(tile[k][q]), tile[k + 1][q]))
                    y = apply(1, x)
                    for q in range(2):
                        first, second = y[2 * q], y[2 * q + 1]
                        a = jnp.where(low, first, swap_halves(second))
                        b = jnp.where(low, swap_halves(first), second)
                        lanes_out = slice(g * LANES, g * LANES + width_at)
                        out_ref[v, 16 * k + 8 * q : 16 * k + 8 * q + 8, lanes_out] = a[:, :width_at]
                        out_ref[v, 16 * (k + 1) + 8 * q : 16 * (k + 1) + 8 * q + 8, lanes_out] = b[:, :width_at]
                return carry

            lax.fori_loop(0, 5, one, 0)


def add_kernel(*refs):
    total = refs[0][...]
    for ref in refs[1:-1]:
        total = total + ref[...]
    refs[-1][...] = total


VMEM = pl.BlockSpec(memory_space=pltpu.MemorySpace.VMEM)
SMEM = pl.BlockSpec(memory_space=pltpu.MemorySpace.SMEM)


def call(body, outs, specs, scratch, name):
    return pl.pallas_call(
        body,
        out_shape=tuple(jax.ShapeDtypeStruct(s, F32) for s in outs),
        in_specs=specs,
        out_specs=tuple(VMEM for _ in outs),
        scratch_shapes=scratch,
        name=name,
    )


def shards(nodal_state, inverse_jacobian, speeds, refine_flags, send_index, face_source):
    elements = nodal_state.shape[2]
    groups = elements // LANES
    total = lax.axis_size("curve")
    half = total // 2
    idx = send_index.reshape(1, -1)
    jac = inverse_jacobian.reshape(groups, LANES)
    flags = refine_flags.reshape(groups, LANES)
    degrees = np.arange(4)
    top = (np.maximum(np.maximum(degrees[:, None, None], degrees[None, :, None]), degrees) == 3).reshape(64, 1)
    kron = np.kron(MODES, np.kron(MODES, MODES))
    modes = jnp.asarray(np.concatenate([kron, np.repeat(top, 64, axis=1)], axis=1), F32)

    sends = call(
        send_kernel,
        [(88, LANES)] * 4,
        [VMEM] * 4,
        [pltpu.VMEM((640, elements), BF), pltpu.VMEM((20, 64, LANES), F32)],
        "send",
    )(nodal_state, idx, jac, flags)
    received = [None] * 4
    for b, o in enumerate(OFFSETS):
        pairs = [(i, (i + o) % total) for i in range(total)]
        received[3 - b] = lax.ppermute(sends[b], "curve", pairs)

    base, slab, outside = call(
        local_kernel,
        [(5 * groups, 64, LANES), (5 * groups, 64, LANES), (6, 80, elements)],
        [VMEM, VMEM, VMEM, SMEM, VMEM],
        [pltpu.VMEM((160, elements), BF), pltpu.VMEM((2 * groups, 8, LANES), F32)],
        "local",
    )(nodal_state, jac, face_source, speeds, modes)

    head, tail, width = call(
        face_kernel,
        [(5 * groups // 2, 64, LANES), (5 * groups // 2, 64, LANES), (16, LANES)],
        [VMEM] * 5 + [SMEM] + [VMEM] * 5,
        [pltpu.VMEM((160, 4 * LANES), BF), pltpu.VMEM((6, 80, elements), F32)],
        "faces",
    )(base, slab, outside, face_source, jac, speeds, flags, *received)

    from_lower = lax.ppermute(tail, "curve", [(i, i + 1) for i in range(total - 1)])
    from_upper = lax.ppermute(head, "curve", [(i + 1, i) for i in range(total - 1)])

    own = width
    reach = 3
    while reach < half:
        shifts = (reach,) if 2 * reach >= half else (reach, 2 * reach)
        parts = [width]
        for s in shifts:
            pairs = [(i, i + s) for i in range(half - s)]
            pairs += [(i, i - s) for i in range(half + s, total)]
            parts.append(lax.ppermute(width, "curve", pairs))
        width = call(add_kernel, [(16, LANES)], [VMEM] * len(parts), [], "add")(*parts)[0]
        reach *= len(shifts) + 1

    state, new_jac = call(
        refine_kernel,
        [(5, 64, E_NEW), (1, E_NEW)],
        [VMEM] * 10,
        [
            pltpu.VMEM((656, 8 * LANES), BF),
            pltpu.VMEM((5, 64, LANES), F32),
            pltpu.VMEM((48, 8, LANES), F32),
            pltpu.VMEM((2, 8 * LANES, LANES), F32),
        ],
        "refine",
    )(from_lower, head, tail, from_upper, width, own, received[1], received[2], jac, flags)
    return state, new_jac.reshape(E_NEW)


def solution(mesh):
    return jax.shard_map(
        shards,
        mesh=mesh,
        in_specs=(
            P(None, None, "curve"),
            P("curve"),
            P(),
            P("curve"),
            P("curve"),
            P(None, "curve"),
        ),
        out_specs=(P(None, None, "curve"), P("curve")),
        check_vma=False,
    )
```

```python
import math

import jax
import jax.numpy as jnp
import numpy as np
from jax import lax
from jax.experimental import pallas as pl
from jax.experimental.pallas import tpu as pltpu
from jax.sharding import PartitionSpec as P

E_NEW = 960
TIME_STEP = 0.02
OFFSETS = (-2, -1, 1, 2)
LANES = 128
BF = jnp.bfloat16
F32 = jnp.float32


def lagrange_at(points, targets):
    values_at = np.ones((len(targets), 4))
    for basis_id in range(4):
        for partner in range(4):
            if partner != basis_id:
                values_at[:, basis_id] *= (targets - points[partner]) / (
                    points[basis_id] - points[partner]
                )
    return values_at


def modes_table(points):
    return np.linalg.inv(np.polynomial.legendre.legvander(points, 3))


def node_constants():
    root = 1.0 / math.sqrt(5.0)
    points = np.array([-1.0, -root, root, 1.0])
    deriv = np.zeros((4, 4))
    bary = np.array([1.0 / np.prod([points[r] - points[c] for c in range(4) if c != r]) for r in range(4)])
    for r in range(4):
        for c in range(4):
            if r != c:
                deriv[r, c] = bary[c] / bary[r] / (points[r] - points[c])
        deriv[r, r] = -np.sum(deriv[r])
    sides = (lagrange_at(points, (points - 1.0) / 2.0), lagrange_at(points, (points + 1.0) / 2.0))
    return deriv, modes_table(points), sides


DERIV, MODES, SIDES = node_constants()
INV_W = (6.0, 1.2, 1.2, 6.0)
SELF_SURFACE = (-3.0, 0.0, 0.0, 3.0)


def low_half(shape=(8, LANES)):
    return lax.broadcasted_iota(jnp.int32, shape, 0) < 4


def swap_halves(x):
    return pltpu.roll(x, 4, axis=0)


def trace_of(ref, t, face):
    dim, side = face // 2, face % 2
    if dim == 0:
        return ref[t, pl.ds(3 * side, 16, stride=4), :]
    if dim == 2:
        return ref[t, 48 * side : 48 * side + 16, :]
    low = low_half()
    tiles = [ref[t, 16 * k + 8 * side : 16 * k + 8 * side + 8, :] for k in range(4)]
    halves = []
    for k in (0, 2):
        if side == 0:
            halves.append(jnp.where(low, tiles[k], swap_halves(tiles[k + 1])))
        else:
            halves.append(jnp.where(low, swap_halves(tiles[k]), tiles[k + 1]))
    return jnp.concatenate(halves, axis=0)


def add_to_face(ref, t, face, value):
    dim, side = face // 2, face % 2
    if dim == 0:
        where_at = (t, pl.ds(3 * side, 16, stride=4), slice(None))
        ref[where_at] = ref[where_at] + value
    elif dim == 2:
        where_at = (t, slice(48 * side, 48 * side + 16), slice(None))
        ref[where_at] = ref[where_at] + value
    else:
        low = low_half()
        keep = low if side == 0 else jnp.logical_not(low)
        for k in range(4):
            half = value[8 * (k // 2) : 8 * (k // 2) + 8, :]
            if (k % 2) != side:
                half = swap_halves(half)
            where_at = (t, slice(16 * k + 8 * side, 16 * k + 8 * side + 8), slice(None))
            ref[where_at] = ref[where_at] + jnp.where(keep, half, 0.0)


def split_two(x):
    high = x.astype(BF)
    return high, (x - high.astype(F32)).astype(BF)


def one_hot(row, count):
    ids = lax.broadcasted_iota(jnp.int32, (count, row.shape[1]), 0)
    return jnp.where(ids == row, 1.0, 0.0).astype(BF)


def dot32(a, b):
    return jnp.dot(a, b, preferred_element_type=F32)


def send_kernel(u_ref, idx_ref, jac_ref, flag_ref, *rest):
    outs, lhs, gathered = rest[:4], rest[4], rest[5]
    elements = u_ref.shape[2]
    slots = idx_ref.shape[0] * LANES // 4
    for v in range(5):
        high, low = split_two(u_ref[v])
        lhs[v * 64 : (v + 1) * 64, :] = high
        lhs[320 + v * 64 : 320 + (v + 1) * 64, :] = low
    row = jnp.concatenate([idx_ref[r : r + 1, :] for r in range(idx_ref.shape[0])], axis=1)
    row = jnp.broadcast_to(row, (8, 4 * slots))
    row = jnp.concatenate([row, jnp.zeros((8, 512 - 4 * slots), jnp.int32)], axis=1)
    blocks = [row[:, :LANES]]
    for b in range(1, 4):
        blocks.append(pltpu.roll(row, 512 - slots * b, axis=1)[:, :LANES])
    idx = jnp.concatenate(blocks, axis=1)
    face = jnp.zeros_like(idx)
    for f in range(1, 6):
        face = face + (idx >= f * elements).astype(jnp.int32)
    elem = idx - face * elements
    picked = dot32(lhs[...], one_hot(elem[0:1], elements))
    for b in range(4):
        part = picked[:320, b * LANES : (b + 1) * LANES] + picked[320:, b * LANES : (b + 1) * LANES]
        gathered[b * 5 : (b + 1) * 5] = part.reshape(5, 64, LANES)
    flags = flag_ref[...].astype(F32)
    count = elements + 7.0 * jnp.sum(flags)
    rows = lax.broadcasted_iota(jnp.int32, (8, LANES), 0)
    groups = elements // LANES
    for b in range(4):
        fb = jnp.broadcast_to(face[0:1, b * LANES : (b + 1) * LANES], (16, LANES))
        for v in range(5):
            value = trace_of(gathered, b * 5 + v, 0)
            for f in range(1, 6):
                value = jnp.where(fb == f, trace_of(gathered, b * 5 + v, f), value)
            outs[b][v * 16 : (v + 1) * 16, :] = value
        near = 0 if OFFSETS[b] < 0 else groups - 2
        meta = jnp.full((8, LANES), count, F32)
        for r in range(2):
            meta = jnp.where(rows == r, jac_ref[near + r : near + r + 1, :], meta)
            meta = jnp.where(rows == 2 + r, flags[near + r : near + r + 1, :], meta)
        outs[b][80:88, :] = meta


def line_rates(x, speed, blend):
    square = [x[m] * x[m] for m in range(4)]
    prod = {}
    for m in range(4):
        for n in range(m + 1, 4):
            prod[m, n] = x[m] * x[n]
    half_speed = 0.5 * jnp.abs(speed)
    flux = []
    for m in range(3):
        central = square[m] + prod[m, m + 1] + square[m + 1]
        reach = jnp.maximum(jnp.abs(x[m]), jnp.abs(x[m + 1]))
        flux.append((speed / 6.0) * central - half_speed * reach * (x[m + 1] - x[m]))
    out = []
    for n in range(4):
        high = None
        diag = -2.0 * DERIV[n, n] / 3.0 + SELF_SURFACE[n]
        for m in range(4):
            if m != n:
                pair = prod[min(m, n), max(m, n)] + square[m]
                term = float(-DERIV[n, m] / 3.0) * pair
                high = term if high is None else high + term
        if n in (0, 3):
            high = high + float(diag) * square[n]
        high = speed * high
        if n == 0:
            low = -INV_W[0] * flux[0]
        elif n == 3:
            low = INV_W[3] * flux[2]
        else:
            low = INV_W[n] * (flux[n - 1] - flux[n])
        out.append(high + blend * (low - high))
    return out


def local_kernel(u_ref, jac_ref, fs_ref, sp_ref, modes_ref, base_ref, slab_ref, out_ref, lhs, rows_s):
    elements = u_ref.shape[2]
    groups = elements // LANES
    for v in range(5):
        for g in range(groups):
            slab_ref[g * 5 + v] = u_ref[v, :, g * LANES : (g + 1) * LANES]
    modal = jnp.dot(
        modes_ref[:, :64], u_ref[0], precision=lax.Precision.HIGHEST, preferred_element_type=F32
    )
    energy = modal * modal
    top = jnp.sum(energy * modes_ref[:, 64:65], axis=0, keepdims=True)
    whole = jnp.sum(energy, axis=0, keepdims=True)
    ratio = top / (whole + 1e-06)
    blend_all = 0.5 * ratio / (ratio + 0.1)
    for g in range(groups):
        rows_s[g] = jnp.broadcast_to(blend_all[:, g * LANES : (g + 1) * LANES], (8, LANES))
        rows_s[groups + g] = jnp.broadcast_to(jac_ref[g : g + 1, :] * TIME_STEP, (8, LANES))

    def one(t, carry):
        g = t // 5
        v = t - 5 * g
        blend = rows_s[g]
        scale = rows_s[groups + g]
        low = low_half()
        for kh in range(2):
            at = [(t, pl.ds(32 * kh + i, 8, stride=4), slice(None)) for i in range(4)]
            rate = line_rates([slab_ref[a] for a in at], sp_ref[0, v], blend)
            for i in range(4):
                base_ref[at[i]] = rate[i]
        tile = [[slab_ref[t, 16 * k + 8 * h : 16 * k + 8 * h + 8, :] for h in range(2)] for k in range(4)]
        rates = [[None, None] for _ in range(4)]
        for h in range(2):
            r = line_rates([tile[k][h] for k in range(4)], sp_ref[2, v], blend)
            for k in range(4):
                rates[k][h] = r[k]
        for k in (0, 2):
            x = []
            for h in range(2):
                x.append(jnp.where(low, tile[k][h], swap_halves(tile[k + 1][h])))
                x.append(jnp.where(low, swap_halves(tile[k][h]), tile[k + 1][h]))
            r = line_rates(x, sp_ref[1, v], blend)
            for h in range(2):
                first, second = r[2 * h], r[2 * h + 1]
                rates[k][h] = rates[k][h] + jnp.where(low, first, swap_halves(second))
                rates[k + 1][h] = rates[k + 1][h] + jnp.where(low, swap_halves(first), second)
        for k in range(4):
            for h in range(2):
                at = (t, slice(16 * k + 8 * h, 16 * k + 8 * h + 8), slice(None))
                base_ref[at] = tile[k][h] + scale * (rates[k][h] + base_ref[at])
        return carry

    lax.fori_loop(0, 5 * groups, one, 0)

    for f in range(6):
        partner = f + 1 - 2 * (f % 2)
        for g in range(groups):
            for v in range(5):
                high, low = split_two(trace_of(slab_ref, g * 5 + v, partner))
                lhs[v * 16 : (v + 1) * 16, g * LANES : (g + 1) * LANES] = high
                lhs[80 + v * 16 : 80 + (v + 1) * 16, g * LANES : (g + 1) * LANES] = low
        picked = dot32(lhs[...], one_hot(fs_ref[f : f + 1, :] - partner * elements, elements))
        near = fs_ref[f : f + 1, :] < 6 * elements
        out_ref[f] = jnp.where(near, picked[:80] + picked[80:], 0.0)


def face_kernel(base_ref, slab_ref, out_ref, fs_ref, jac_ref, sp_ref, flag_ref, r0, r1, r2, r3, *rest):
    head_ref, tail_ref, width_ref, lhs, outside = rest
    elements = fs_ref.shape[1]
    groups = elements // LANES
    slots = 96
    for b, ref in enumerate((r0, r1, r2, r3)):
        high, low = split_two(ref[0:80, :])
        lhs[0:80, b * LANES : (b + 1) * LANES] = high
        lhs[80:160, b * LANES : (b + 1) * LANES] = low
    half = 5 * (groups // 2)
    head_ref[...] = base_ref[0:half]
    tail_ref[...] = base_ref[half : 2 * half]
    for f in range(6):
        ghost = fs_ref[f : f + 1, :] - 6 * elements
        place = jnp.zeros_like(ghost)
        for b in range(1, 4):
            place = place + (ghost >= b * slots).astype(jnp.int32)
        column = ghost + place * (LANES - slots)
        picked = dot32(lhs[...], one_hot(column, 4 * LANES))
        outside[f] = out_ref[f] + (picked[:80] + picked[80:])
    for g in range(groups):
        ref, first = (head_ref, 0) if g < groups // 2 else (tail_ref, groups // 2)
        scale = jnp.broadcast_to(jac_ref[g : g + 1, :] * TIME_STEP, (16, LANES))
        for v in range(5):
            t = g * 5 + v
            for f in range(6):
                speed = sp_ref[f // 2, v]
                inner = trace_of(slab_ref, t, f)
                outer = outside[f, v * 16 : (v + 1) * 16, g * LANES : (g + 1) * LANES]
                central = inner * inner + inner * outer + outer * outer
                reach = (3.0 * jnp.abs(speed)) * jnp.maximum(jnp.abs(inner), jnp.abs(outer))
                sign = 1.0 if f % 2 == 0 else -1.0
                value = (sign * speed) * central - reach * (inner - outer)
                add_to_face(ref, (g - first) * 5 + v, f, scale * value)
    me = lax.axis_index("curve")
    total = lax.axis_size("curve")
    lower = me < total // 2
    count = jnp.full((8, LANES), elements + 7.0 * jnp.sum(flag_ref[...].astype(F32)), F32)
    own = count
    for o, ref in zip(OFFSETS, (r0, r1, r2, r3)):
        there = me + o
        wanted = jnp.logical_and(lower if o < 0 else jnp.logical_not(lower), jnp.logical_and(there >= 0, there < total))
        value = jnp.broadcast_to(ref[87:88, :], (8, LANES))
        count = count + value * jnp.where(wanted, 1.0, 0.0)
    width_ref[0:8] = count
    width_ref[8:16] = own


def refine_kernel(low_ref, head_ref, tail_ref, up_ref, w_ref, own_ref, r1, r2, jac_ref, flag_ref, *rest):
    out_ref, jout_ref, lhs, res, coef, cols = rest
    halves = (low_ref, head_ref, tail_ref, up_ref)
    total = lax.axis_size("curve")
    me = lax.axis_index("curve")
    for b, ref in enumerate(halves):
        for g in range(2):
            high, low = split_two(ref[5 * g : 5 * g + 5].reshape(320, LANES))
            at = slice((2 * b + g) * LANES, (2 * b + g + 1) * LANES)
            lhs[0:320, at] = high
            lhs[320:640, at] = low
    jac = jnp.concatenate([r1[80:82, :], jac_ref[...], r2[80:82, :]], axis=0)
    flag = jnp.concatenate([r1[82:84, :], flag_ref[...].astype(F32), r2[82:84, :]], axis=0)
    sizes = 1.0 + 7.0 * flag
    lane0 = lax.broadcasted_iota(jnp.int32, (LANES, LANES), 0)
    lane1 = lax.broadcasted_iota(jnp.int32, (LANES, LANES), 1)
    upper = jnp.where(lane0 < lane1, 1.0, 0.0).astype(BF)
    sizes_b = sizes.astype(BF)
    within = dot32(sizes_b, upper)
    row_total = jnp.sum(sizes, axis=1, keepdims=True)
    running = jnp.zeros((1, 1), F32)
    starts = []
    for r in range(8):
        starts.append(running)
        running = running + row_total[r : r + 1]
    row0 = lax.broadcasted_iota(jnp.int32, (8, LANES), 0)
    before = within
    for r in range(8):
        before = before + jnp.where(row0 == r, starts[r], 0.0)
    width = w_ref[0:8]
    if own_ref is not None:
        width = width
    mine = own_ref[8:16]
    lower = jnp.where(me < total // 2, 1.0, 0.0)
    begin = lower * (width - mine) + (1.0 - lower) * (float(total * E_NEW) - width)
    begin = begin - (me * E_NEW).astype(F32)
    place = before + (begin - starts[2])
    ends = place + sizes
    place_hi = jnp.floor(place * (1.0 / 256.0))
    place_lo = place - 256.0 * place_hi
    jac_a = jac.astype(BF)
    jac_b = (jac - jac_a.astype(F32)).astype(BF)
    jac_c = (jac - jac_a.astype(F32) - jac_b.astype(F32)).astype(BF)
    rows16 = lax.broadcasted_iota(jnp.int32, (16, LANES), 0)
    extras = [jac_a.astype(F32), jac_b.astype(F32), jac_c.astype(F32), flag, place_hi, place_lo]
    for r in range(8):
        block = jnp.zeros((16, LANES), F32)
        for q, item in enumerate(extras):
            block = jnp.where(rows16 == q, jnp.broadcast_to(item[r : r + 1, :], (16, LANES)), block)
        lhs[640:656, r * LANES : (r + 1) * LANES] = block.astype(BF)
        cols[0, r * LANES : (r + 1) * LANES, :] = jnp.transpose(jnp.broadcast_to(place[r : r + 1, :], (LANES, LANES)))
        cols[1, r * LANES : (r + 1) * LANES, :] = jnp.transpose(jnp.broadcast_to(ends[r : r + 1, :], (LANES, LANES)))

    spans = ((0, 768), (256, 768), (256, 1024), (256, 1024))
    for pair, (k0, k1) in enumerate(spans):
        pieces = []
        for h in range(2):
            slot = (lax.broadcasted_iota(jnp.int32, (8, LANES), 1) + (2 * pair + h) * LANES).astype(F32)
            slot_b = jnp.broadcast_to(slot[0:1], (k1 - k0, LANES))
            hit = jnp.logical_and(slot_b >= cols[0, k0:k1, :], slot_b < cols[1, k0:k1, :])
            pieces.append(jnp.where(hit, 1.0, 0.0).astype(BF))
        picked = dot32(lhs[:, k0:k1], jnp.concatenate(pieces, axis=1))
        for h in range(2):
            g = 2 * pair + h
            lanes = slice(h * LANES, (h + 1) * LANES)
            width_at = min(LANES, E_NEW - g * LANES)
            res[...] = (picked[0:320, lanes] + picked[320:640, lanes]).reshape(5, 64, LANES)
            extra = picked[640:656, lanes]
            jac_new = (extra[0:1] + extra[1:2] + extra[2:3]) * (1.0 + extra[3:4])
            jout_ref[0:1, g * LANES : g * LANES + width_at] = jac_new[:, :width_at]
            fl = jnp.broadcast_to(extra[3:4], (8, LANES))
            slot = (lax.broadcasted_iota(jnp.int32, (8, LANES), 1) + g * LANES).astype(F32)
            child = slot - (256.0 * extra[4:5] + extra[5:6])
            bit2 = jnp.where(child >= 4.0, 1.0, 0.0)
            child = child - 4.0 * bit2
            bit1 = jnp.where(child >= 2.0, 1.0, 0.0)
            bit0 = child - 2.0 * bit1
            for d, bit in enumerate((bit0, bit1, bit2)):
                both = fl * bit
                for i in range(4):
                    for m in range(4):
                        eye = 1.0 if i == m else 0.0
                        c = fl * float(SIDES[0][i, m] - eye) + both * float(SIDES[1][i, m] - SIDES[0][i, m]) + eye
                        coef[16 * d + 4 * i + m] = c

            def apply(d, x):
                out = []
                for i in range(4):
                    acc = coef[16 * d + 4 * i] * x[0]
                    for m in range(1, 4):
                        acc = acc + coef[16 * d + 4 * i + m] * x[m]
                    out.append(acc)
                return out

            def one(v, carry):
                low = low_half()
                for kh in range(2):
                    at = [(v, pl.ds(32 * kh + i, 8, stride=4), slice(None)) for i in range(4)]
                    y = apply(0, [res[a] for a in at])
                    for i in range(4):
                        res[at[i]] = y[i]
                tile = [[res[v, 16 * k + 8 * q : 16 * k + 8 * q + 8, :] for q in range(2)] for k in range(4)]
                for q in range(2):
                    y = apply(2, [tile[k][q] for k in range(4)])
                    for k in range(4):
                        tile[k][q] = y[k]
                for k in (0, 2):
                    x = []
                    for q in range(2):
                        x.append(jnp.where(low, tile[k][q], swap_halves(tile[k + 1][q])))
                        x.append(jnp.where(low, swap_halves(tile[k][q]), tile[k + 1][q]))
                    y = apply(1, x)
                    for q in range(2):
                        first, second = y[2 * q], y[2 * q + 1]
                        a = jnp.where(low, first, swap_halves(second))
                        b = jnp.where(low, swap_halves(first), second)
                        lanes_out = slice(g * LANES, g * LANES + width_at)
                        out_ref[v, 16 * k + 8 * q : 16 * k + 8 * q + 8, lanes_out] = a[:, :width_at]
                        out_ref[v, 16 * (k + 1) + 8 * q : 16 * (k + 1) + 8 * q + 8, lanes_out] = b[:, :width_at]
                return carry

            lax.fori_loop(0, 5, one, 0)


def add_kernel(*refs):
    total = refs[0][...]
    for ref in refs[1:-1]:
        total = total + ref[...]
    refs[-1][...] = total


VMEM = pl.BlockSpec(memory_space=pltpu.MemorySpace.VMEM)
SMEM = pl.BlockSpec(memory_space=pltpu.MemorySpace.SMEM)


def call(body, outs, specs, scratch, name):
    return pl.pallas_call(
        body,
        out_shape=tuple(jax.ShapeDtypeStruct(s, F32) for s in outs),
        in_specs=specs,
        out_specs=tuple(VMEM for _ in outs),
        scratch_shapes=scratch,
        name=name,
        compiler_params=pltpu.CompilerParams(vmem_limit_bytes=16 << 20),
    )


def shards(nodal_state, inverse_jacobian, speeds, refine_flags, send_index, face_source):
    elements = nodal_state.shape[2]
    groups = elements // LANES
    total = lax.axis_size("curve")
    half = total // 2
    idx = send_index.reshape(-1, LANES)
    jac = inverse_jacobian.reshape(groups, LANES)
    flags = refine_flags.reshape(groups, LANES)
    degrees = np.arange(4)
    top = (np.maximum(np.maximum(degrees[:, None, None], degrees[None, :, None]), degrees) == 3).reshape(64, 1)
    kron = np.kron(MODES, np.kron(MODES, MODES))
    modes = jnp.asarray(np.concatenate([kron, np.repeat(top, 64, axis=1)], axis=1), F32)

    sends = call(
        send_kernel,
        [(88, LANES)] * 4,
        [VMEM] * 4,
        [pltpu.VMEM((640, elements), BF), pltpu.VMEM((20, 64, LANES), F32)],
        "send",
    )(nodal_state, idx, jac, flags)
    received = [None] * 4
    for b, o in enumerate(OFFSETS):
        pairs = [(i, (i + o) % total) for i in range(total)]
        received[3 - b] = lax.ppermute(sends[b], "curve", pairs)

    base, slab, outside = call(
        local_kernel,
        [(5 * groups, 64, LANES), (5 * groups, 64, LANES), (6, 80, elements)],
        [VMEM, VMEM, VMEM, SMEM, VMEM],
        [pltpu.VMEM((160, elements), BF), pltpu.VMEM((2 * groups, 8, LANES), F32)],
        "local",
    )(nodal_state, jac, face_source, speeds, modes)

    head, tail, width = call(
        face_kernel,
        [(5 * groups // 2, 64, LANES), (5 * groups // 2, 64, LANES), (16, LANES)],
        [VMEM] * 5 + [SMEM] + [VMEM] * 5,
        [pltpu.VMEM((160, 4 * LANES), BF), pltpu.VMEM((6, 80, elements), F32)],
        "faces",
    )(base, slab, outside, face_source, jac, speeds, flags, *received)

    from_lower = lax.ppermute(tail, "curve", [(i, i + 1) for i in range(total - 1)])
    from_upper = lax.ppermute(head, "curve", [(i + 1, i) for i in range(total - 1)])

    own = width
    reach = 3
    while reach < half:
        shifts = (reach,) if 2 * reach >= half else (reach, 2 * reach)
        parts = [width]
        for s in shifts:
            pairs = [(i, i + s) for i in range(half - s)]
            pairs += [(i, i - s) for i in range(half + s, total)]
            parts.append(lax.ppermute(width, "curve", pairs))
        width = call(add_kernel, [(16, LANES)], [VMEM] * len(parts), [], "add")(*parts)[0]
        reach *= len(shifts) + 1

    state, new_jac = call(
        refine_kernel,
        [(5, 64, E_NEW), (1, E_NEW)],
        [VMEM] * 10,
        [
            pltpu.VMEM((656, 8 * LANES), BF),
            pltpu.VMEM((5, 64, LANES), F32),
            pltpu.VMEM((48, 8, LANES), F32),
            pltpu.VMEM((2, 8 * LANES, LANES), F32),
        ],
        "refine",
    )(from_lower, head, tail, from_upper, width, own, received[1], received[2], jac, flags)
    return state, new_jac.reshape(E_NEW)


def solution(mesh):
    return jax.shard_map(
        shards,
        mesh=mesh,
        in_specs=(
            P(None, None, "curve"),
            P("curve"),
            P(),
            P("curve"),
            P("curve"),
            P(None, "curve"),
        ),
        out_specs=(P(None, None, "curve"), P("curve")),
        check_vma=False,
    )
```

```python
import math

import jax
import jax.numpy as jnp
import numpy as np
from jax import lax
from jax.experimental import pallas as pl
from jax.experimental.pallas import tpu as pltpu
from jax.sharding import PartitionSpec as P

E_NEW = 960
TIME_STEP = 0.02
OFFSETS = (-2, -1, 1, 2)
LANES = 128
BF = jnp.bfloat16
F32 = jnp.float32


def lagrange_at(points, targets):
    values_at = np.ones((len(targets), 4))
    for basis_id in range(4):
        for partner in range(4):
            if partner != basis_id:
                values_at[:, basis_id] *= (targets - points[partner]) / (
                    points[basis_id] - points[partner]
                )
    return values_at


def modes_table(points):
    return np.linalg.inv(np.polynomial.legendre.legvander(points, 3))


def node_constants():
    root = 1.0 / math.sqrt(5.0)
    points = np.array([-1.0, -root, root, 1.0])
    deriv = np.zeros((4, 4))
    bary = np.array([1.0 / np.prod([points[r] - points[c] for c in range(4) if c != r]) for r in range(4)])
    for r in range(4):
        for c in range(4):
            if r != c:
                deriv[r, c] = bary[c] / bary[r] / (points[r] - points[c])
        deriv[r, r] = -np.sum(deriv[r])
    sides = (lagrange_at(points, (points - 1.0) / 2.0), lagrange_at(points, (points + 1.0) / 2.0))
    return deriv, modes_table(points), sides


DERIV, MODES, SIDES = node_constants()
INV_W = (6.0, 1.2, 1.2, 6.0)
SELF_SURFACE = (-3.0, 0.0, 0.0, 3.0)


def low_half(shape=(8, LANES)):
    return lax.broadcasted_iota(jnp.int32, shape, 0) < 4


def swap_halves(x):
    return pltpu.roll(x, 4, axis=0)


def trace_of(ref, t, face):
    dim, side = face // 2, face % 2
    if dim == 0:
        return ref[t, pl.ds(3 * side, 16, stride=4), :]
    if dim == 2:
        return ref[t, 48 * side : 48 * side + 16, :]
    low = low_half()
    tiles = [ref[t, 16 * k + 8 * side : 16 * k + 8 * side + 8, :] for k in range(4)]
    halves = []
    for k in (0, 2):
        if side == 0:
            halves.append(jnp.where(low, tiles[k], swap_halves(tiles[k + 1])))
        else:
            halves.append(jnp.where(low, swap_halves(tiles[k]), tiles[k + 1]))
    return jnp.concatenate(halves, axis=0)


def add_to_face(ref, t, face, value):
    dim, side = face // 2, face % 2
    if dim == 0:
        where_at = (t, pl.ds(3 * side, 16, stride=4), slice(None))
        ref[where_at] = ref[where_at] + value
    elif dim == 2:
        where_at = (t, slice(48 * side, 48 * side + 16), slice(None))
        ref[where_at] = ref[where_at] + value
    else:
        low = low_half()
        keep = low if side == 0 else jnp.logical_not(low)
        for k in range(4):
            half = value[8 * (k // 2) : 8 * (k // 2) + 8, :]
            if (k % 2) != side:
                half = swap_halves(half)
            where_at = (t, slice(16 * k + 8 * side, 16 * k + 8 * side + 8), slice(None))
            ref[where_at] = ref[where_at] + jnp.where(keep, half, 0.0)


def split_two(x):
    high = x.astype(BF)
    return high, (x - high.astype(F32)).astype(BF)


def one_hot(row, count):
    ids = lax.broadcasted_iota(jnp.int32, (count, row.shape[1]), 0)
    return jnp.where(ids == row, 1.0, 0.0).astype(BF)


def dot32(a, b):
    return jnp.dot(a, b, preferred_element_type=F32)


def send_kernel(u_hbm, idx_hbm, jac_hbm, flag_hbm, fs_hbm, sp_hbm, modes_hbm, *rest):
    outs = rest[:4]
    slab_ref, jac_ref, flag_ref, fs_ref, speed_ref, modes_ref = rest[4:10]
    lhs, gathered, idx_ref, flag_raw, sp_ref, sems = rest[10:]
    elements = u_hbm.shape[2]
    groups = elements // LANES
    loads = [pltpu.make_async_copy(idx_hbm, idx_ref, sems.at[0])]
    for g in range(groups):
        for v in range(5):
            loads.append(
                pltpu.make_async_copy(
                    u_hbm.at[v, :, pl.ds(g * LANES, LANES)], slab_ref.at[g * 5 + v], sems.at[len(loads)]
                )
            )
    for src, dst in (
        (jac_hbm, jac_ref),
        (flag_hbm, flag_raw),
        (fs_hbm, fs_ref),
        (sp_hbm, sp_ref),
        (modes_hbm, modes_ref),
    ):
        loads.append(pltpu.make_async_copy(src, dst, sems.at[len(loads)]))
    for load in loads:
        load.start()
    loads[0].wait()
    slots = idx_ref.shape[0] * LANES // 4
    row = jnp.concatenate([idx_ref[r : r + 1, :] for r in range(idx_ref.shape[0])], axis=1)
    row = jnp.broadcast_to(row, (8, 4 * slots))
    row = jnp.concatenate([row, jnp.zeros((8, 512 - 4 * slots), jnp.int32)], axis=1)
    blocks = [row[:, :LANES]]
    for b in range(1, 4):
        blocks.append(pltpu.roll(row, 512 - slots * b, axis=1)[:, :LANES])
    idx = jnp.concatenate(blocks, axis=1)
    face = jnp.zeros_like(idx)
    for f in range(1, 6):
        face = face + (idx >= f * elements).astype(jnp.int32)
    elem = idx - face * elements
    wanted = one_hot(elem[0:1], elements)
    for g in range(groups):
        for v in range(5):
            loads[1 + g * 5 + v].wait()
            high, low = split_two(slab_ref[g * 5 + v])
            lanes = slice(g * LANES, (g + 1) * LANES)
            lhs[v * 64 : (v + 1) * 64, lanes] = high
            lhs[320 + v * 64 : 320 + (v + 1) * 64, lanes] = low
    picked = dot32(lhs[...], wanted)
    for b in range(4):
        part = picked[:320, b * LANES : (b + 1) * LANES] + picked[320:, b * LANES : (b + 1) * LANES]
        gathered[b * 5 : (b + 1) * 5] = part.reshape(5, 64, LANES)
    for load in loads[1 + 5 * groups :]:
        load.wait()
    flags = flag_raw[...].astype(F32)
    flag_ref[...] = flags
    count = elements + 7.0 * jnp.sum(flags)
    rows = lax.broadcasted_iota(jnp.int32, (8, LANES), 0)
    for b in range(4):
        fb = jnp.broadcast_to(face[0:1, b * LANES : (b + 1) * LANES], (16, LANES))
        for v in range(5):
            value = trace_of(gathered, b * 5 + v, 0)
            for f in range(1, 6):
                value = jnp.where(fb == f, trace_of(gathered, b * 5 + v, f), value)
            outs[b][v * 16 : (v + 1) * 16, :] = value
        near = 0 if OFFSETS[b] < 0 else groups - 2
        meta = jnp.full((8, LANES), count, F32)
        for r in range(2):
            meta = jnp.where(rows == r, jac_ref[near + r : near + r + 1, :], meta)
            meta = jnp.where(rows == 2 + r, flags[near + r : near + r + 1, :], meta)
        outs[b][80:88, :] = meta
    for d in range(3):
        for v in range(5):
            speed_ref[d * 5 + v] = jnp.broadcast_to(sp_ref[d : d + 1, v : v + 1], (16, LANES))


def line_rates(x, speed, blend):
    square = [x[m] * x[m] for m in range(4)]
    prod = {}
    for m in range(4):
        for n in range(m + 1, 4):
            prod[m, n] = x[m] * x[n]
    half_speed = 0.5 * jnp.abs(speed)
    flux = []
    for m in range(3):
        central = square[m] + prod[m, m + 1] + square[m + 1]
        reach = jnp.maximum(jnp.abs(x[m]), jnp.abs(x[m + 1]))
        flux.append((speed / 6.0) * central - half_speed * reach * (x[m + 1] - x[m]))
    out = []
    for n in range(4):
        high = None
        diag = -2.0 * DERIV[n, n] / 3.0 + SELF_SURFACE[n]
        for m in range(4):
            if m != n:
                pair = prod[min(m, n), max(m, n)] + square[m]
                term = float(-DERIV[n, m] / 3.0) * pair
                high = term if high is None else high + term
        if n in (0, 3):
            high = high + float(diag) * square[n]
        high = speed * high
        if n == 0:
            low = -INV_W[0] * flux[0]
        elif n == 3:
            low = INV_W[3] * flux[2]
        else:
            low = INV_W[n] * (flux[n - 1] - flux[n])
        out.append(high + blend * (low - high))
    return out


def local_kernel(slab_ref, jac_ref, sp_ref, modes_ref, base_ref, first, rows_s):
    groups = jac_ref.shape[0]
    for g in range(groups):
        first[:, g * LANES : (g + 1) * LANES] = slab_ref[g * 5]
    modal = jnp.dot(
        modes_ref[:, :64], first[...], precision=lax.Precision.HIGHEST, preferred_element_type=F32
    )
    energy = modal * modal
    top = jnp.sum(energy * modes_ref[:, 64:65], axis=0, keepdims=True)
    whole = jnp.sum(energy, axis=0, keepdims=True)
    ratio = top / (whole + 1e-06)
    blend_all = 0.5 * ratio / (ratio + 0.1)
    for g in range(groups):
        rows_s[g] = jnp.broadcast_to(blend_all[:, g * LANES : (g + 1) * LANES], (8, LANES))
        rows_s[groups + g] = jnp.broadcast_to(jac_ref[g : g + 1, :] * TIME_STEP, (8, LANES))

    def one(t, carry):
        g = t // 5
        v = t - 5 * g
        blend = rows_s[g]
        scale = rows_s[groups + g]
        low = low_half()
        speeds = [sp_ref[5 * d + v, 0:8, :] for d in range(3)]
        for kh in range(2):
            at = [(t, pl.ds(32 * kh + i, 8, stride=4), slice(None)) for i in range(4)]
            rate = line_rates([slab_ref[a] for a in at], speeds[0], blend)
            for i in range(4):
                base_ref[at[i]] = rate[i]
        tile = [[slab_ref[t, 16 * k + 8 * h : 16 * k + 8 * h + 8, :] for h in range(2)] for k in range(4)]
        rates = [[None, None] for _ in range(4)]
        for h in range(2):
            r = line_rates([tile[k][h] for k in range(4)], speeds[2], blend)
            for k in range(4):
                rates[k][h] = r[k]
        for k in (0, 2):
            x = []
            for h in range(2):
                x.append(jnp.where(low, tile[k][h], swap_halves(tile[k + 1][h])))
                x.append(jnp.where(low, swap_halves(tile[k][h]), tile[k + 1][h]))
            r = line_rates(x, speeds[1], blend)
            for h in range(2):
                one_row, two_row = r[2 * h], r[2 * h + 1]
                rates[k][h] = rates[k][h] + jnp.where(low, one_row, swap_halves(two_row))
                rates[k + 1][h] = rates[k + 1][h] + jnp.where(low, swap_halves(one_row), two_row)
        for k in range(4):
            for h in range(2):
                at = (t, slice(16 * k + 8 * h, 16 * k + 8 * h + 8), slice(None))
                base_ref[at] = tile[k][h] + scale * (rates[k][h] + base_ref[at])
        return carry

    lax.fori_loop(0, 5 * groups, one, 0)


def outside_kernel(slab_ref, fs_ref, after_ref, out_ref, lhs):
    del after_ref
    elements = fs_ref.shape[1]
    groups = elements // LANES
    for f in range(6):
        partner = f + 1 - 2 * (f % 2)
        for g in range(groups):
            for v in range(5):
                high, low = split_two(trace_of(slab_ref, g * 5 + v, partner))
                lhs[v * 16 : (v + 1) * 16, g * LANES : (g + 1) * LANES] = high
                lhs[80 + v * 16 : 80 + (v + 1) * 16, g * LANES : (g + 1) * LANES] = low
        picked = dot32(lhs[...], one_hot(fs_ref[f : f + 1, :] - partner * elements, elements))
        near = fs_ref[f : f + 1, :] < 6 * elements
        out_ref[f] = jnp.where(near, picked[:80] + picked[80:], 0.0)


def window_kernel(flag_ref, after_ref, r0, r1, r2, r3, width_ref):
    del after_ref
    me = lax.axis_index("curve")
    total = lax.axis_size("curve")
    lower = me < total // 2
    elements = flag_ref.shape[0] * LANES
    count = jnp.full((8, LANES), elements + 7.0 * jnp.sum(flag_ref[...]), F32)
    own = count
    for o, ref in zip(OFFSETS, (r0, r1, r2, r3)):
        there = me + o
        wanted = jnp.logical_and(lower if o < 0 else jnp.logical_not(lower), jnp.logical_and(there >= 0, there < total))
        value = jnp.broadcast_to(ref[87:88, :], (8, LANES))
        count = count + value * jnp.where(wanted, 1.0, 0.0)
    width_ref[0:8] = count
    width_ref[8:16] = own


def face_kernel(base_ref, slab_ref, out_ref, fs_ref, jac_ref, sp_ref, after_ref, r0, r1, r2, r3, *rest):
    del after_ref
    head_ref, tail_ref, lhs, outside = rest
    elements = fs_ref.shape[1]
    groups = elements // LANES
    slots = 96
    for b, ref in enumerate((r0, r1, r2, r3)):
        high, low = split_two(ref[0:80, :])
        lhs[0:80, b * LANES : (b + 1) * LANES] = high
        lhs[80:160, b * LANES : (b + 1) * LANES] = low
    half = 5 * (groups // 2)
    head_ref[...] = base_ref[0:half]
    tail_ref[...] = base_ref[half : 2 * half]
    for f in range(6):
        ghost = fs_ref[f : f + 1, :] - 6 * elements
        place = jnp.zeros_like(ghost)
        for b in range(1, 4):
            place = place + (ghost >= b * slots).astype(jnp.int32)
        column = ghost + place * (LANES - slots)
        picked = dot32(lhs[...], one_hot(column, 4 * LANES))
        outside[f] = out_ref[f] + (picked[:80] + picked[80:])
    for g in range(groups):
        ref, first = (head_ref, 0) if g < groups // 2 else (tail_ref, groups // 2)
        scale = jnp.broadcast_to(jac_ref[g : g + 1, :] * TIME_STEP, (16, LANES))
        for v in range(5):
            t = g * 5 + v
            for f in range(6):
                speed = sp_ref[5 * (f // 2) + v]
                inner = trace_of(slab_ref, t, f)
                outer = outside[f, v * 16 : (v + 1) * 16, g * LANES : (g + 1) * LANES]
                central = inner * inner + inner * outer + outer * outer
                reach = (3.0 * jnp.abs(speed)) * jnp.maximum(jnp.abs(inner), jnp.abs(outer))
                sign = 1.0 if f % 2 == 0 else -1.0
                value = (sign * speed) * central - reach * (inner - outer)
                add_to_face(ref, (g - first) * 5 + v, f, scale * value)


EDGE_GROUPS = (0, 1, 5, 6, 7)
SPANS = ((0, 768), (256, 768), (256, 1024), (256, 1024))


def interpolate(res, v, coef, first, store):
    def apply(d, x):
        out = []
        for i in range(4):
            acc = coef[first + 16 * d + 4 * i] * x[0]
            for m in range(1, 4):
                acc = acc + coef[first + 16 * d + 4 * i + m] * x[m]
            out.append(acc)
        return out

    low = low_half()
    for kh in range(2):
        at = [(v, pl.ds(32 * kh + i, 8, stride=4), slice(None)) for i in range(4)]
        y = apply(0, [res[a] for a in at])
        for i in range(4):
            res[at[i]] = y[i]
    tile = [[res[v, 16 * k + 8 * q : 16 * k + 8 * q + 8, :] for q in range(2)] for k in range(4)]
    for q in range(2):
        y = apply(2, [tile[k][q] for k in range(4)])
        for k in range(4):
            tile[k][q] = y[k]
    for k in (0, 2):
        x = []
        for q in range(2):
            x.append(jnp.where(low, tile[k][q], swap_halves(tile[k + 1][q])))
            x.append(jnp.where(low, swap_halves(tile[k][q]), tile[k + 1][q]))
        y = apply(1, x)
        for q in range(2):
            one_row, two_row = y[2 * q], y[2 * q + 1]
            store(16 * k + 8 * q, jnp.where(low, one_row, swap_halves(two_row)))
            store(16 * (k + 1) + 8 * q, jnp.where(low, swap_halves(one_row), two_row))


def own_kernel(head_ref, tail_ref, w_ref, own_ref, r1, r2, jac_ref, flag_ref, *rest):
    mid_ref, part_ref, low_hot, up_hot, coef_out, jout_ref = rest[:6]
    lhs, meta, res, coef_mid, cols = rest[6:]
    total = lax.axis_size("curve")
    me = lax.axis_index("curve")
    for b, ref in enumerate((head_ref, tail_ref)):
        for g in range(2):
            high, low = split_two(ref[5 * g : 5 * g + 5].reshape(320, LANES))
            at = slice((2 * b + g) * LANES, (2 * b + g + 1) * LANES)
            lhs[0:320, at] = high
            lhs[320:640, at] = low
    jac = jnp.concatenate([r1[80:82, :], jac_ref[...], r2[80:82, :]], axis=0)
    flag = jnp.concatenate([r1[82:84, :], flag_ref[...], r2[82:84, :]], axis=0)
    sizes = 1.0 + 7.0 * flag
    lane0 = lax.broadcasted_iota(jnp.int32, (LANES, LANES), 0)
    lane1 = lax.broadcasted_iota(jnp.int32, (LANES, LANES), 1)
    upper = jnp.where(lane0 < lane1, 1.0, 0.0).astype(BF)
    before = dot32(sizes.astype(BF), upper)
    row_total = jnp.sum(sizes, axis=1, keepdims=True)
    running = jnp.zeros((1, 1), F32)
    starts = []
    for r in range(8):
        starts.append(running)
        running = running + row_total[r : r + 1]
    row0 = lax.broadcasted_iota(jnp.int32, (8, LANES), 0)
    for r in range(8):
        before = before + jnp.where(row0 == r, starts[r], 0.0)
    width = w_ref[0:8]
    mine = own_ref[8:16]
    lower = jnp.where(me < total // 2, 1.0, 0.0)
    begin = lower * (width - mine) + (1.0 - lower) * (float(total * E_NEW) - width)
    begin = begin - (me * E_NEW).astype(F32)
    place = before + (begin - starts[2])
    ends = place + sizes
    place_hi = jnp.floor(place * (1.0 / 256.0))
    place_lo = place - 256.0 * place_hi
    jac_a = jac.astype(BF)
    jac_b = (jac - jac_a.astype(F32)).astype(BF)
    jac_c = (jac - jac_a.astype(F32) - jac_b.astype(F32)).astype(BF)
    rows16 = lax.broadcasted_iota(jnp.int32, (16, LANES), 0)
    extras = [jac_a.astype(F32), jac_b.astype(F32), jac_c.astype(F32), flag, place_hi, place_lo]
    for r in range(8):
        block = jnp.zeros((16, LANES), F32)
        for q, item in enumerate(extras):
            block = jnp.where(rows16 == q, jnp.broadcast_to(item[r : r + 1, :], (16, LANES)), block)
        at = slice(r * LANES, (r + 1) * LANES)
        meta[:, at] = block.astype(BF)
        cols[0, at, :] = jnp.transpose(jnp.broadcast_to(place[r : r + 1, :], (LANES, LANES)))
        cols[1, at, :] = jnp.transpose(jnp.broadcast_to(ends[r : r + 1, :], (LANES, LANES)))

    for pair, (k0, k1) in enumerate(SPANS):
        pieces = []
        for h in range(2):
            slot = (lax.broadcasted_iota(jnp.int32, (8, LANES), 1) + (2 * pair + h) * LANES).astype(F32)
            slot_b = jnp.broadcast_to(slot[0:1], (k1 - k0, LANES))
            hit = jnp.logical_and(slot_b >= cols[0, k0:k1, :], slot_b < cols[1, k0:k1, :])
            pieces.append(jnp.where(hit, 1.0, 0.0).astype(BF))
        hot = jnp.concatenate(pieces, axis=1)
        if pair == 0:
            low_hot[...] = hot[0:256]
        elif pair == 2:
            up_hot[:, 0:LANES] = hot[512:768, LANES : 2 * LANES]
        elif pair == 3:
            up_hot[:, LANES : 3 * LANES] = hot[512:768]
        picked = dot32(lhs[...], hot[256 - k0 : 768 - k0])
        known = dot32(meta[:, k0:k1], hot)
        for h in range(2):
            g = 2 * pair + h
            lanes = slice(h * LANES, (h + 1) * LANES)
            width_at = min(LANES, E_NEW - g * LANES)
            extra = known[:, lanes]
            jac_new = (extra[0:1] + extra[1:2] + extra[2:3]) * (1.0 + extra[3:4])
            jout_ref[0:1, g * LANES : g * LANES + width_at] = jac_new[:, :width_at]
            fl = jnp.broadcast_to(extra[3:4], (8, LANES))
            slot = (lax.broadcasted_iota(jnp.int32, (8, LANES), 1) + g * LANES).astype(F32)
            child = slot - (256.0 * extra[4:5] + extra[5:6])
            bit2 = jnp.where(child >= 4.0, 1.0, 0.0)
            child = child - 4.0 * bit2
            bit1 = jnp.where(child >= 2.0, 1.0, 0.0)
            bit0 = child - 2.0 * bit1
            edge = g in EDGE_GROUPS
            coef, first = (coef_out, 48 * EDGE_GROUPS.index(g)) if edge else (coef_mid, 48 * (g - 2))
            for d, bit in enumerate((bit0, bit1, bit2)):
                both = fl * bit
                for i in range(4):
                    for m in range(4):
                        eye = 1.0 if i == m else 0.0
                        c = fl * float(SIDES[0][i, m] - eye) + both * float(SIDES[1][i, m] - SIDES[0][i, m]) + eye
                        coef[first + 16 * d + 4 * i + m] = c
            value = (picked[0:320, lanes] + picked[320:640, lanes]).reshape(5, 64, LANES)
            if edge:
                q = EDGE_GROUPS.index(g)
                part_ref[5 * q : 5 * q + 5] = value
            else:
                res[...] = value

                def one(v, carry, g=g, first=first):
                    def store(row, x):
                        mid_ref[5 * (g - 2) + v, row : row + 8, :] = x

                    interpolate(res, v, coef_mid, first, store)
                    return carry

                lax.fori_loop(0, 5, one, 0)


def edge_kernel(low_ref, up_ref, mid_ref, part_ref, low_hot, up_hot, coef_ref, out_hbm, lhs, res, out, sems):
    for b, ref in enumerate((low_ref, up_ref)):
        for g in range(2):
            high, low = split_two(ref[5 * g : 5 * g + 5].reshape(320, LANES))
            at = slice((2 * b + g) * LANES, (2 * b + g + 1) * LANES)
            lhs[0:320, at] = high
            lhs[320:640, at] = low
    picked = (dot32(lhs[:, 0:256], low_hot[...]), dot32(lhs[:, 256:512], up_hot[...]))
    for q, g in enumerate(EDGE_GROUPS):
        from_up = int(g >= 5)
        at = (g - 5 * from_up) * LANES
        value = picked[from_up][0:320, at : at + LANES] + picked[from_up][320:640, at : at + LANES]
        res[5 * q : 5 * q + 5] = part_ref[5 * q : 5 * q + 5] + value.reshape(5, 64, LANES)
    for v in range(5):
        for g in (2, 3, 4):
            out[v, :, g * LANES : (g + 1) * LANES] = mid_ref[5 * (g - 2) + v]
        for q, g in enumerate(EDGE_GROUPS):
            width_at = min(LANES, E_NEW - g * LANES)

            def store(row, x, v=v, g=g, width_at=width_at):
                out[v, row : row + 8, g * LANES : g * LANES + width_at] = x[:, :width_at]

            interpolate(res, 5 * q + v, coef_ref, 48 * q, store)
        pltpu.make_async_copy(out.at[v], out_hbm.at[v], sems.at[v]).start()
    for v in range(5):
        pltpu.make_async_copy(out.at[v], out_hbm.at[v], sems.at[v]).wait()


def add_kernel(*refs):
    total = refs[0][...]
    for ref in refs[1:-1]:
        total = total + ref[...]
    refs[-1][...] = total


VMEM = pl.BlockSpec(memory_space=pltpu.MemorySpace.VMEM)
HBM = pl.BlockSpec(memory_space=pltpu.MemorySpace.HBM)


def in_hbm(x):
    return pltpu.with_memory_space_constraint(x, pltpu.MemorySpace.HBM)


def call(body, outs, specs, scratch, name, out_spec=VMEM, flops=100_000_000):
    shapes = []
    for item in outs:
        shape, dtype = item if isinstance(item[0], tuple) else (item, F32)
        shapes.append(jax.ShapeDtypeStruct(shape, dtype))
    return pl.pallas_call(
        body,
        out_shape=tuple(shapes),
        in_specs=specs,
        out_specs=tuple(out_spec for _ in outs),
        scratch_shapes=scratch,
        name=name,
        compiler_params=pltpu.CompilerParams(vmem_limit_bytes=16 << 20),
    )


def shards(nodal_state, inverse_jacobian, speeds, refine_flags, send_index, face_source):
    elements = nodal_state.shape[2]
    groups = elements // LANES
    total = lax.axis_size("curve")
    half = total // 2
    idx = send_index.reshape(-1, LANES)
    jac = inverse_jacobian.reshape(groups, LANES)
    flags = refine_flags.reshape(groups, LANES)
    degrees = np.arange(4)
    top = (np.maximum(np.maximum(degrees[:, None, None], degrees[None, :, None]), degrees) == 3).reshape(64, 1)
    kron = np.kron(MODES, np.kron(MODES, MODES))
    modes = jnp.asarray(np.concatenate([kron, np.repeat(top, 64, axis=1)], axis=1), F32)
    slabs = 5 * groups

    outs = call(
        send_kernel,
        [(88, LANES)] * 4
        + [
            (slabs, 64, LANES),
            (groups, LANES),
            (groups, LANES),
            ((6, elements), jnp.int32),
            (15, 16, LANES),
            (64, LANES),
        ],
        [HBM] * 7,
        [
            pltpu.VMEM((640, elements), BF),
            pltpu.VMEM((20, 64, LANES), F32),
            pltpu.VMEM(idx.shape, jnp.int32),
            pltpu.VMEM((groups, LANES), jnp.int32),
            pltpu.VMEM(speeds.shape, F32),
            pltpu.SemaphoreType.DMA((slabs + 6,)),
        ],
        "send",
    )(*(in_hbm(x) for x in (nodal_state, idx, jac, flags, face_source, speeds, modes)))
    sends = outs[:4]
    slab, jac, flags, face_source, speeds, modes = outs[4:]
    received = [None] * 4
    for b, o in enumerate(OFFSETS):
        pairs = [(i, (i + o) % total) for i in range(total)]
        received[3 - b] = lax.ppermute(sends[b], "curve", pairs)

    (base,) = call(
        local_kernel,
        [(slabs, 64, LANES)],
        [VMEM] * 4,
        [pltpu.VMEM((64, elements), F32), pltpu.VMEM((2 * groups, 8, LANES), F32)],
        "local",
    )(slab, jac, speeds, modes)

    (width,) = call(window_kernel, [(16, LANES)], [VMEM] * 6, [], "window")(flags, base, *received)
    own = width
    (outside,) = call(
        outside_kernel, [(6, 80, elements)], [VMEM] * 3, [pltpu.VMEM((160, elements), BF)], "outside"
    )(slab, face_source, width)
    after = width
    reach = 3
    while reach < half:
        after = width
        shifts = (reach,) if 2 * reach >= half else (reach, 2 * reach)
        parts = [width]
        for s in shifts:
            pairs = [(i, i + s) for i in range(half - s)]
            pairs += [(i, i - s) for i in range(half + s, total)]
            parts.append(lax.ppermute(width, "curve", pairs))
        (width,) = call(add_kernel, [(16, LANES)], [VMEM] * len(parts), [], "add")(*parts)
        reach *= len(shifts) + 1

    half_slabs = (slabs // 2, 64, LANES)
    head, tail = call(
        face_kernel,
        [half_slabs, half_slabs],
        [VMEM] * 11,
        [pltpu.VMEM((160, 4 * LANES), BF), pltpu.VMEM((6, 80, elements), F32)],
        "faces",
    )(base, slab, outside, face_source, jac, speeds, after, *received)

    from_lower = lax.ppermute(tail, "curve", [(i, i + 1) for i in range(total - 1)])
    from_upper = lax.ppermute(head, "curve", [(i + 1, i) for i in range(total - 1)])

    *kept, new_jac = call(
        own_kernel,
        [
            (15, 64, LANES),
            (25, 64, LANES),
            ((256, 256), BF),
            ((256, 384), BF),
            (5 * 48, 8, LANES),
            (1, E_NEW),
        ],
        [VMEM] * 8,
        [
            pltpu.VMEM((640, elements), BF),
            pltpu.VMEM((16, 8 * LANES), BF),
            pltpu.VMEM((5, 64, LANES), F32),
            pltpu.VMEM((3 * 48, 8, LANES), F32),
            pltpu.VMEM((2, 8 * LANES, LANES), F32),
        ],
        "own",
    )(head, tail, width, own, received[1], received[2], jac, flags)
    (state,) = call(
        edge_kernel,
        [(5, 64, E_NEW)],
        [VMEM] * 7,
        [
            pltpu.VMEM((640, 4 * LANES), BF),
            pltpu.VMEM((25, 64, LANES), F32),
            pltpu.VMEM((5, 64, E_NEW), F32),
            pltpu.SemaphoreType.DMA((5,)),
        ],
        "edge",
        HBM,
    )(from_lower, from_upper, *kept)
    return state, new_jac.reshape(E_NEW)


def solution(mesh):
    return jax.shard_map(
        shards,
        mesh=mesh,
        in_specs=(
            P(None, None, "curve"),
            P("curve"),
            P(),
            P("curve"),
            P("curve"),
            P(None, "curve"),
        ),
        out_specs=(P(None, None, "curve"), P("curve")),
        check_vma=False,
    )
```

```python
import math

import jax
import jax.numpy as jnp
import numpy as np
from jax import lax
from jax.experimental import pallas as pl
from jax.experimental.pallas import tpu as pltpu
from jax.sharding import PartitionSpec as P

E_NEW = 960
TIME_STEP = 0.02
OFFSETS = (-2, -1, 1, 2)
LANES = 128
BF = jnp.bfloat16
F32 = jnp.float32


def lagrange_at(points, targets):
    values_at = np.ones((len(targets), 4))
    for basis_id in range(4):
        for partner in range(4):
            if partner != basis_id:
                values_at[:, basis_id] *= (targets - points[partner]) / (
                    points[basis_id] - points[partner]
                )
    return values_at


def modes_table(points):
    return np.linalg.inv(np.polynomial.legendre.legvander(points, 3))


def node_constants():
    root = 1.0 / math.sqrt(5.0)
    points = np.array([-1.0, -root, root, 1.0])
    deriv = np.zeros((4, 4))
    bary = np.array([1.0 / np.prod([points[r] - points[c] for c in range(4) if c != r]) for r in range(4)])
    for r in range(4):
        for c in range(4):
            if r != c:
                deriv[r, c] = bary[c] / bary[r] / (points[r] - points[c])
        deriv[r, r] = -np.sum(deriv[r])
    sides = (lagrange_at(points, (points - 1.0) / 2.0), lagrange_at(points, (points + 1.0) / 2.0))
    return deriv, modes_table(points), sides


DERIV, MODES, SIDES = node_constants()
INV_W = (6.0, 1.2, 1.2, 6.0)
SELF_SURFACE = (-3.0, 0.0, 0.0, 3.0)


def low_half(shape=(8, LANES)):
    return lax.broadcasted_iota(jnp.int32, shape, 0) < 4


def swap_halves(x):
    return pltpu.roll(x, 4, axis=0)


def position():
    me = lax.axis_index("curve")
    return me, me % 2 == 0, (me // 2) % 2 == 0


def pick(flag, yes, no):
    return jnp.where(flag, yes, no)


def trace_of(ref, t, face):
    dim, side = face // 2, face % 2
    if dim == 0:
        return ref[t, pl.ds(3 * side, 16, stride=4), :]
    if dim == 2:
        return ref[t, 48 * side : 48 * side + 16, :]
    low = low_half()
    tiles = [ref[t, 16 * k + 8 * side : 16 * k + 8 * side + 8, :] for k in range(4)]
    halves = []
    for k in (0, 2):
        if side == 0:
            halves.append(jnp.where(low, tiles[k], swap_halves(tiles[k + 1])))
        else:
            halves.append(jnp.where(low, swap_halves(tiles[k]), tiles[k + 1]))
    return jnp.concatenate(halves, axis=0)


def add_to_face(ref, first, face, value):
    dim, side = face // 2, face % 2
    if dim == 0:
        where_at = (pl.ds(first + 3 * side, 16, stride=4), slice(None))
        ref[where_at] = ref[where_at] + value
    elif dim == 2:
        where_at = (slice(first + 48 * side, first + 48 * side + 16), slice(None))
        ref[where_at] = ref[where_at] + value
    else:
        low = low_half()
        keep = low if side == 0 else jnp.logical_not(low)
        for k in range(4):
            half = value[8 * (k // 2) : 8 * (k // 2) + 8, :]
            if (k % 2) != side:
                half = swap_halves(half)
            where_at = (slice(first + 16 * k + 8 * side, first + 16 * k + 8 * side + 8), slice(None))
            ref[where_at] = ref[where_at] + jnp.where(keep, half, 0.0)


def split_two(x):
    high = x.astype(BF)
    return high, (x - high.astype(F32)).astype(BF)


def one_hot(row, count):
    ids = lax.broadcasted_iota(jnp.int32, (count, row.shape[1]), 0)
    return jnp.where(ids == row, 1.0, 0.0).astype(BF)


def dot32(a, b):
    return jnp.dot(a, b, preferred_element_type=F32)


def send_kernel(u_hbm, idx_hbm, jac_hbm, flag_hbm, fs_hbm, sp_hbm, modes_hbm, *rest):
    outs = rest[:4]
    slab_ref, jac_ref, flag_ref, fs_ref, speed_ref, modes_ref = rest[4:10]
    lhs, gathered, faces, idx_ref, flag_raw, sp_ref, sems = rest[10:]
    elements = u_hbm.shape[2]
    groups = elements // LANES
    loads = [pltpu.make_async_copy(idx_hbm, idx_ref, sems.at[0])]
    for g in range(groups):
        for v in range(5):
            loads.append(
                pltpu.make_async_copy(
                    u_hbm.at[v, :, pl.ds(g * LANES, LANES)], slab_ref.at[g * 5 + v], sems.at[len(loads)]
                )
            )
    for src, dst in (
        (jac_hbm, jac_ref),
        (flag_hbm, flag_raw),
        (fs_hbm, fs_ref),
        (sp_hbm, sp_ref),
        (modes_hbm, modes_ref),
    ):
        loads.append(pltpu.make_async_copy(src, dst, sems.at[len(loads)]))
    for load in loads:
        load.start()
    loads[0].wait()
    slots = idx_ref.shape[0] * LANES // 4
    row = jnp.concatenate([idx_ref[r : r + 1, :] for r in range(idx_ref.shape[0])], axis=1)
    row = jnp.broadcast_to(row, (8, 4 * slots))
    row = jnp.concatenate([row, jnp.zeros((8, 512 - 4 * slots), jnp.int32)], axis=1)
    blocks = [row[:, :LANES]]
    for b in range(1, 4):
        blocks.append(pltpu.roll(row, 512 - slots * b, axis=1)[:, :LANES])
    idx = jnp.concatenate(blocks, axis=1)
    face = jnp.zeros_like(idx)
    for f in range(1, 6):
        face = face + (idx >= f * elements).astype(jnp.int32)
    elem = idx - face * elements
    wanted = one_hot(elem[0:1], elements)
    for g in range(groups):
        for v in range(5):
            loads[1 + g * 5 + v].wait()
            high, low = split_two(slab_ref[g * 5 + v])
            lanes = slice(g * LANES, (g + 1) * LANES)
            lhs[v * 64 : (v + 1) * 64, lanes] = high
            lhs[320 + v * 64 : 320 + (v + 1) * 64, lanes] = low
    picked = dot32(lhs[...], wanted)
    for b in range(4):
        part = picked[:320, b * LANES : (b + 1) * LANES] + picked[320:, b * LANES : (b + 1) * LANES]
        gathered[b * 5 : (b + 1) * 5] = part.reshape(5, 64, LANES)
    for load in loads[1 + 5 * groups :]:
        load.wait()
    flags = flag_raw[...].astype(F32)
    flag_ref[...] = flags
    count = elements + 7.0 * jnp.sum(flags)
    rows = lax.broadcasted_iota(jnp.int32, (8, LANES), 0)
    for b in range(4):
        faces[b] = jnp.broadcast_to(face[0:1, b * LANES : (b + 1) * LANES], (16, LANES))
    me, even, even_chip = position()
    sent = (pick(even, 2, 1), pick(even, 1, 2), pick(even_chip, 3, 0), pick(even_chip, 0, 3))
    for q, b in enumerate(sent):
        fb = faces[b]
        for v in range(5):
            value = trace_of(gathered, b * 5 + v, 0)
            for f in range(1, 6):
                value = jnp.where(fb == f, trace_of(gathered, b * 5 + v, f), value)
            outs[q][v * 16 : (v + 1) * 16, :] = value
        last = b >= 2
        meta = jnp.full((8, LANES), count, F32)
        for r in range(2):
            far = groups - 2 + r
            meta = jnp.where(rows == r, pick(last, jac_ref[far : far + 1, :], jac_ref[r : r + 1, :]), meta)
            meta = jnp.where(rows == 2 + r, pick(last, flags[far : far + 1, :], flags[r : r + 1, :]), meta)
        outs[q][80:88, :] = meta
    for d in range(3):
        for v in range(5):
            speed_ref[d * 5 + v] = jnp.broadcast_to(sp_ref[d : d + 1, v : v + 1], (16, LANES))


def line_rates(x, speed, blend):
    square = [x[m] * x[m] for m in range(4)]
    prod = {}
    for m in range(4):
        for n in range(m + 1, 4):
            prod[m, n] = x[m] * x[n]
    half_speed = 0.5 * jnp.abs(speed)
    flux = []
    for m in range(3):
        central = square[m] + prod[m, m + 1] + square[m + 1]
        reach = jnp.maximum(jnp.abs(x[m]), jnp.abs(x[m + 1]))
        flux.append((speed / 6.0) * central - half_speed * reach * (x[m + 1] - x[m]))
    out = []
    for n in range(4):
        high = None
        diag = -2.0 * DERIV[n, n] / 3.0 + SELF_SURFACE[n]
        for m in range(4):
            if m != n:
                pair = prod[min(m, n), max(m, n)] + square[m]
                term = float(-DERIV[n, m] / 3.0) * pair
                high = term if high is None else high + term
        if n in (0, 3):
            high = high + float(diag) * square[n]
        high = speed * high
        if n == 0:
            low = -INV_W[0] * flux[0]
        elif n == 3:
            low = INV_W[3] * flux[2]
        else:
            low = INV_W[n] * (flux[n - 1] - flux[n])
        out.append(high + blend * (low - high))
    return out


def local_kernel(slab_ref, jac_ref, sp_ref, modes_ref, base_ref, first, rows_s):
    groups = jac_ref.shape[0]
    for g in range(groups):
        first[:, g * LANES : (g + 1) * LANES] = slab_ref[g * 5]
    modal = jnp.dot(
        modes_ref[:, :64], first[...], precision=lax.Precision.HIGHEST, preferred_element_type=F32
    )
    energy = modal * modal
    top = jnp.sum(energy * modes_ref[:, 64:65], axis=0, keepdims=True)
    whole = jnp.sum(energy, axis=0, keepdims=True)
    ratio = top / (whole + 1e-06)
    blend_all = 0.5 * ratio / (ratio + 0.1)
    for g in range(groups):
        rows_s[g] = jnp.broadcast_to(blend_all[:, g * LANES : (g + 1) * LANES], (8, LANES))
        rows_s[groups + g] = jnp.broadcast_to(jac_ref[g : g + 1, :] * TIME_STEP, (8, LANES))

    def one(t, carry):
        g = t // 5
        v = t - 5 * g
        blend = rows_s[g]
        scale = rows_s[groups + g]
        low = low_half()
        speeds = [sp_ref[5 * d + v, 0:8, :] for d in range(3)]
        for kh in range(2):
            at = [(t, pl.ds(32 * kh + i, 8, stride=4), slice(None)) for i in range(4)]
            rate = line_rates([slab_ref[a] for a in at], speeds[0], blend)
            for i in range(4):
                base_ref[at[i]] = rate[i]
        tile = [[slab_ref[t, 16 * k + 8 * h : 16 * k + 8 * h + 8, :] for h in range(2)] for k in range(4)]
        rates = [[None, None] for _ in range(4)]
        for h in range(2):
            r = line_rates([tile[k][h] for k in range(4)], speeds[2], blend)
            for k in range(4):
                rates[k][h] = r[k]
        for k in (0, 2):
            x = []
            for h in range(2):
                x.append(jnp.where(low, tile[k][h], swap_halves(tile[k + 1][h])))
                x.append(jnp.where(low, swap_halves(tile[k][h]), tile[k + 1][h]))
            r = line_rates(x, speeds[1], blend)
            for h in range(2):
                one_row, two_row = r[2 * h], r[2 * h + 1]
                rates[k][h] = rates[k][h] + jnp.where(low, one_row, swap_halves(two_row))
                rates[k + 1][h] = rates[k + 1][h] + jnp.where(low, swap_halves(one_row), two_row)
        for k in range(4):
            for h in range(2):
                at = (t, slice(16 * k + 8 * h, 16 * k + 8 * h + 8), slice(None))
                base_ref[at] = tile[k][h] + scale * (rates[k][h] + base_ref[at])
        return carry

    lax.fori_loop(0, 5 * groups, one, 0)


def outside_kernel(slab_ref, fs_ref, out_ref, lhs):
    elements = fs_ref.shape[1]
    groups = elements // LANES
    for f in range(6):
        partner = f + 1 - 2 * (f % 2)
        for g in range(groups):
            for v in range(5):
                high, low = split_two(trace_of(slab_ref, g * 5 + v, partner))
                lhs[v * 16 : (v + 1) * 16, g * LANES : (g + 1) * LANES] = high
                lhs[80 + v * 16 : 80 + (v + 1) * 16, g * LANES : (g + 1) * LANES] = low
        picked = dot32(lhs[...], one_hot(fs_ref[f : f + 1, :] - partner * elements, elements))
        near = fs_ref[f : f + 1, :] < 6 * elements
        value = jnp.where(near, picked[:80] + picked[80:], 0.0)
        for g in range(groups):
            out_ref[f * groups + g] = value[:, g * LANES : (g + 1) * LANES]


def ghost_kernel(out_ref, fs_ref, after_ref, rd, rb, rc, ra, full_ref, lhs):
    del after_ref
    elements = fs_ref.shape[1]
    groups = elements // LANES
    slots = 96
    me, even, even_chip = position()
    spots = (pick(even, 2, 1), pick(even, 1, 2), pick(even_chip, 3, 0), pick(even_chip, 0, 3))
    for spot, ref in zip(spots, (ra, rb, rc, rd)):
        high, low = split_two(ref[0:80, :])
        lanes = pl.ds(pl.multiple_of(spot * LANES, LANES), LANES)
        lhs[0:80, lanes] = high
        lhs[80:160, lanes] = low
    for f in range(6):
        ghost = fs_ref[f : f + 1, :] - 6 * elements
        place = jnp.zeros_like(ghost)
        for b in range(1, 4):
            place = place + (ghost >= b * slots).astype(jnp.int32)
        column = ghost + place * (LANES - slots)
        picked = dot32(lhs[...], one_hot(column, 4 * LANES))
        picked = picked[:80] + picked[80:]
        for g in range(groups):
            full_ref[f * groups + g] = out_ref[f * groups + g] + picked[:, g * LANES : (g + 1) * LANES]


def face_kernel(base_ref, slab_ref, full_ref, jac_ref, sp_ref, flag_ref, first_ref, second_ref, counts_ref, scales):
    groups = jac_ref.shape[0]
    half = groups // 2
    me, even, _ = position()
    for g in range(groups):
        scales[g] = jnp.broadcast_to(jac_ref[g : g + 1, :] * TIME_STEP, (16, LANES))
    for ref, start in ((first_ref, pick(even, half, 0)), (second_ref, pick(even, 0, half))):
        for i in range(half):
            g = start + i
            scale = scales[g]
            for v in range(5):
                t = g * 5 + v
                row = (i * 5 + v) * 64
                ref[row : row + 64, :] = base_ref[t]
                for f in range(6):
                    speed = sp_ref[5 * (f // 2) + v]
                    inner = trace_of(slab_ref, t, f)
                    outer = full_ref[f * groups + g, v * 16 : (v + 1) * 16, :]
                    central = inner * inner + inner * outer + outer * outer
                    reach = (3.0 * jnp.abs(speed)) * jnp.maximum(jnp.abs(inner), jnp.abs(outer))
                    sign = 1.0 if f % 2 == 0 else -1.0
                    value = (sign * speed) * central - reach * (inner - outer)
                    add_to_face(ref, row, f, scale * value)
    counts_ref[...] = jnp.full(counts_ref.shape, groups * LANES + 7.0 * jnp.sum(flag_ref[...]), F32)


EDGE_GROUPS = (0, 1, 5, 6, 7)
SPANS = ((0, 768), (256, 768), (256, 1024), (256, 1024))


def interpolate(res, v, coef, first, store):
    def apply(d, x):
        out = []
        for i in range(4):
            acc = coef[first + 16 * d + 4 * i] * x[0]
            for m in range(1, 4):
                acc = acc + coef[first + 16 * d + 4 * i + m] * x[m]
            out.append(acc)
        return out

    low = low_half()
    for kh in range(2):
        at = [(v, pl.ds(32 * kh + i, 8, stride=4), slice(None)) for i in range(4)]
        y = apply(0, [res[a] for a in at])
        for i in range(4):
            res[at[i]] = y[i]
    tile = [[res[v, 16 * k + 8 * q : 16 * k + 8 * q + 8, :] for q in range(2)] for k in range(4)]
    for q in range(2):
        y = apply(2, [tile[k][q] for k in range(4)])
        for k in range(4):
            tile[k][q] = y[k]
    for k in (0, 2):
        x = []
        for q in range(2):
            x.append(jnp.where(low, tile[k][q], swap_halves(tile[k + 1][q])))
            x.append(jnp.where(low, swap_halves(tile[k][q]), tile[k + 1][q]))
        y = apply(1, x)
        for q in range(2):
            one_row, two_row = y[2 * q], y[2 * q + 1]
            store(16 * k + 8 * q, jnp.where(low, one_row, swap_halves(two_row)))
            store(16 * (k + 1) + 8 * q, jnp.where(low, swap_halves(one_row), two_row))


def own_kernel(first_ref, second_ref, counts_ref, ra, rb, jac_ref, flag_ref, *rest):
    mid_ref, part_ref, low_hot, up_hot, coef_out, jout_ref = rest[:6]
    lhs, meta, res, coef_mid, cols = rest[6:]
    me, even, _ = position()
    for ref, start in ((first_ref, pick(even, 2, 0)), (second_ref, pick(even, 0, 2))):
        for g in range(2):
            high, low = split_two(ref[320 * g : 320 * g + 320, :])
            at = pl.ds(pl.multiple_of((start + g) * LANES, LANES), LANES)
            lhs[0:320, at] = high
            lhs[320:640, at] = low
    near_a, near_b = ra[80:88, :], rb[80:88, :]
    below, above = pick(even, near_b, near_a), pick(even, near_a, near_b)
    jac = jnp.concatenate([below[0:2], jac_ref[...], above[0:2]], axis=0)
    flag = jnp.concatenate([below[2:4], flag_ref[...], above[2:4]], axis=0)
    sizes = 1.0 + 7.0 * flag
    lane0 = lax.broadcasted_iota(jnp.int32, (LANES, LANES), 0)
    lane1 = lax.broadcasted_iota(jnp.int32, (LANES, LANES), 1)
    upper = jnp.where(lane0 < lane1, 1.0, 0.0).astype(BF)
    before = dot32(sizes.astype(BF), upper)
    row_total = jnp.sum(sizes, axis=1, keepdims=True)
    running = jnp.zeros((1, 1), F32)
    starts = []
    for r in range(8):
        starts.append(running)
        running = running + row_total[r : r + 1]
    row0 = lax.broadcasted_iota(jnp.int32, (8, LANES), 0)
    for r in range(8):
        before = before + jnp.where(row0 == r, starts[r], 0.0)
    counts = counts_ref[...]
    half = counts.shape[0]
    upper = me >= half
    earlier = lax.broadcasted_iota(jnp.int32, counts.shape, 0) < me % half
    begin = jnp.sum(jnp.where(earlier, counts, 0.0), axis=0, keepdims=True)
    rest = float(2 * half * E_NEW) - jnp.sum(counts, axis=0, keepdims=True)
    begin = begin + pick(upper, rest, jnp.zeros_like(rest))
    begin = begin - (me * E_NEW).astype(F32)
    place = before + (begin - starts[2])
    ends = place + sizes
    place_hi = jnp.floor(place * (1.0 / 256.0))
    place_lo = place - 256.0 * place_hi
    jac_a = jac.astype(BF)
    jac_b = (jac - jac_a.astype(F32)).astype(BF)
    jac_c = (jac - jac_a.astype(F32) - jac_b.astype(F32)).astype(BF)
    rows16 = lax.broadcasted_iota(jnp.int32, (16, LANES), 0)
    extras = [jac_a.astype(F32), jac_b.astype(F32), jac_c.astype(F32), flag, place_hi, place_lo]
    for r in range(8):
        block = jnp.zeros((16, LANES), F32)
        for q, item in enumerate(extras):
            block = jnp.where(rows16 == q, jnp.broadcast_to(item[r : r + 1, :], (16, LANES)), block)
        at = slice(r * LANES, (r + 1) * LANES)
        meta[:, at] = block.astype(BF)
        cols[0, at, :] = jnp.transpose(jnp.broadcast_to(place[r : r + 1, :], (LANES, LANES)))
        cols[1, at, :] = jnp.transpose(jnp.broadcast_to(ends[r : r + 1, :], (LANES, LANES)))

    for pair, (k0, k1) in enumerate(SPANS):
        pieces = []
        for h in range(2):
            slot = (lax.broadcasted_iota(jnp.int32, (8, LANES), 1) + (2 * pair + h) * LANES).astype(F32)
            slot_b = jnp.broadcast_to(slot[0:1], (k1 - k0, LANES))
            hit = jnp.logical_and(slot_b >= cols[0, k0:k1, :], slot_b < cols[1, k0:k1, :])
            pieces.append(jnp.where(hit, 1.0, 0.0).astype(BF))
        hot = jnp.concatenate(pieces, axis=1)
        if pair == 0:
            low_hot[...] = hot[0:256]
        elif pair == 2:
            up_hot[:, 0:LANES] = hot[512:768, LANES : 2 * LANES]
        elif pair == 3:
            up_hot[:, LANES : 3 * LANES] = hot[512:768]
        picked = dot32(lhs[...], hot[256 - k0 : 768 - k0])
        known = dot32(meta[:, k0:k1], hot)
        for h in range(2):
            g = 2 * pair + h
            lanes = slice(h * LANES, (h + 1) * LANES)
            width_at = min(LANES, E_NEW - g * LANES)
            extra = known[:, lanes]
            jac_new = (extra[0:1] + extra[1:2] + extra[2:3]) * (1.0 + extra[3:4])
            jout_ref[0:1, g * LANES : g * LANES + width_at] = jac_new[:, :width_at]
            fl = jnp.broadcast_to(extra[3:4], (8, LANES))
            slot = (lax.broadcasted_iota(jnp.int32, (8, LANES), 1) + g * LANES).astype(F32)
            child = slot - (256.0 * extra[4:5] + extra[5:6])
            bit2 = jnp.where(child >= 4.0, 1.0, 0.0)
            child = child - 4.0 * bit2
            bit1 = jnp.where(child >= 2.0, 1.0, 0.0)
            bit0 = child - 2.0 * bit1
            edge = g in EDGE_GROUPS
            coef, first = (coef_out, 48 * EDGE_GROUPS.index(g)) if edge else (coef_mid, 48 * (g - 2))
            for d, bit in enumerate((bit0, bit1, bit2)):
                both = fl * bit
                for i in range(4):
                    for m in range(4):
                        eye = 1.0 if i == m else 0.0
                        c = fl * float(SIDES[0][i, m] - eye) + both * float(SIDES[1][i, m] - SIDES[0][i, m]) + eye
                        coef[first + 16 * d + 4 * i + m] = c
            value = (picked[0:320, lanes] + picked[320:640, lanes]).reshape(5, 64, LANES)
            if edge:
                q = EDGE_GROUPS.index(g)
                part_ref[5 * q : 5 * q + 5] = value
            else:
                res[...] = value

                def one(v, carry, g=g, first=first):
                    def store(row, x):
                        mid_ref[5 * (g - 2) + v, row : row + 8, :] = x

                    interpolate(res, v, coef_mid, first, store)
                    return carry

                lax.fori_loop(0, 5, one, 0)


def edge_kernel(b_ref, a_ref, mid_ref, part_ref, low_hot, up_hot, coef_ref, out_hbm, lhs, res, out, sems):
    _, even, _ = position()
    for ref, start in ((a_ref, pick(even, 2, 0)), (b_ref, pick(even, 0, 2))):
        for g in range(2):
            high, low = split_two(ref[320 * g : 320 * g + 320, :])
            at = pl.ds(pl.multiple_of((start + g) * LANES, LANES), LANES)
            lhs[0:320, at] = high
            lhs[320:640, at] = low
    picked = (dot32(lhs[:, 0:256], low_hot[...]), dot32(lhs[:, 256:512], up_hot[...]))
    for q, g in enumerate(EDGE_GROUPS):
        from_up = int(g >= 5)
        at = (g - 5 * from_up) * LANES
        value = picked[from_up][0:320, at : at + LANES] + picked[from_up][320:640, at : at + LANES]
        res[5 * q : 5 * q + 5] = part_ref[5 * q : 5 * q + 5] + value.reshape(5, 64, LANES)
    for v in range(5):
        for g in (2, 3, 4):
            out[v, :, g * LANES : (g + 1) * LANES] = mid_ref[5 * (g - 2) + v]
        for q, g in enumerate(EDGE_GROUPS):
            width_at = min(LANES, E_NEW - g * LANES)

            def store(row, x, v=v, g=g, width_at=width_at):
                out[v, row : row + 8, g * LANES : g * LANES + width_at] = x[:, :width_at]

            interpolate(res, 5 * q + v, coef_ref, 48 * q, store)
        pltpu.make_async_copy(out.at[v], out_hbm.at[v], sems.at[v]).start()
    for v in range(5):
        pltpu.make_async_copy(out.at[v], out_hbm.at[v], sems.at[v]).wait()


VMEM = pl.BlockSpec(memory_space=pltpu.MemorySpace.VMEM)
HBM = pl.BlockSpec(memory_space=pltpu.MemorySpace.HBM)


def swap(x, pairs):
    return lax.ppermute(x, "curve", list(pairs) + [(b, a) for a, b in pairs])


def in_hbm(x):
    return pltpu.with_memory_space_constraint(x, pltpu.MemorySpace.HBM)


def call(body, outs, specs, scratch, name, out_spec=VMEM, flops=100_000_000):
    shapes = []
    for item in outs:
        shape, dtype = item if isinstance(item[0], tuple) else (item, F32)
        shapes.append(jax.ShapeDtypeStruct(shape, dtype))
    return pl.pallas_call(
        body,
        out_shape=tuple(shapes),
        in_specs=specs,
        out_specs=tuple(out_spec for _ in outs),
        scratch_shapes=scratch,
        name=name,
        compiler_params=pltpu.CompilerParams(vmem_limit_bytes=16 << 20),
    )


def shards(nodal_state, inverse_jacobian, speeds, refine_flags, send_index, face_source):
    elements = nodal_state.shape[2]
    groups = elements // LANES
    total = lax.axis_size("curve")
    half = total // 2
    idx = send_index.reshape(-1, LANES)
    jac = inverse_jacobian.reshape(groups, LANES)
    flags = refine_flags.reshape(groups, LANES)
    degrees = np.arange(4)
    top = (np.maximum(np.maximum(degrees[:, None, None], degrees[None, :, None]), degrees) == 3).reshape(64, 1)
    kron = np.kron(MODES, np.kron(MODES, MODES))
    modes = jnp.asarray(np.concatenate([kron, np.repeat(top, 64, axis=1)], axis=1), F32)
    slabs = 5 * groups

    outs = call(
        send_kernel,
        [(88, LANES)] * 4
        + [
            (slabs, 64, LANES),
            (groups, LANES),
            (groups, LANES),
            ((6, elements), jnp.int32),
            (15, 16, LANES),
            (64, LANES),
        ],
        [HBM] * 7,
        [
            pltpu.VMEM((640, elements), BF),
            pltpu.VMEM((20, 64, LANES), F32),
            pltpu.VMEM((4, 16, LANES), jnp.int32),
            pltpu.VMEM(idx.shape, jnp.int32),
            pltpu.VMEM((groups, LANES), jnp.int32),
            pltpu.VMEM(speeds.shape, F32),
            pltpu.SemaphoreType.DMA((slabs + 6,)),
        ],
        "send",
    )(*(in_hbm(x) for x in (nodal_state, idx, jac, flags, face_source, speeds, modes)))
    sends = outs[:4]
    slab, jac, flags, face_source, speeds, modes = outs[4:]
    pair_a = [(i, i + 1) for i in range(0, total, 2)]
    pair_b = [(i, (i + 1) % total) for i in range(1, total, 2)]
    pair_c = [(i, i + 2) for i in range(total) if (i // 2) % 2 == 0]
    pair_d = [(i, (i + 2) % total) for i in range(total) if (i // 2) % 2 == 1]
    received = [swap(x, pairs) for x, pairs in zip(sends, (pair_a, pair_b, pair_c, pair_d))]

    (base,) = call(
        local_kernel,
        [(slabs, 64, LANES)],
        [VMEM] * 4,
        [pltpu.VMEM((64, elements), F32), pltpu.VMEM((2 * groups, 8, LANES), F32)],
        "local",
    )(slab, jac, speeds, modes)

    (outside,) = call(
        outside_kernel, [(6 * groups, 80, LANES)], [VMEM] * 2, [pltpu.VMEM((160, elements), BF)], "outside"
    )(slab, face_source)
    (full,) = call(
        ghost_kernel, [(6 * groups, 80, LANES)], [VMEM] * 7, [pltpu.VMEM((160, 4 * LANES), BF)], "ghost"
    )(outside, face_source, base, *(received[q] for q in (3, 1, 2, 0)))
    rows = slabs // 2 * 64
    first, second, counts = call(
        face_kernel,
        [(rows, LANES), (rows, LANES), (half, LANES)],
        [VMEM] * 6,
        [pltpu.VMEM((groups, 16, LANES), F32)],
        "faces",
    )(base, slab, full, jac, speeds, flags)

    from_a = swap(first, pair_a)
    from_b = swap(second, pair_b[:-1])

    halves = [list(range(half)), list(range(half, total))]
    counts = lax.all_to_all(counts, "curve", 0, 0, axis_index_groups=halves, tiled=True)

    *kept, new_jac = call(
        own_kernel,
        [
            (15, 64, LANES),
            (25, 64, LANES),
            ((256, 256), BF),
            ((256, 384), BF),
            (5 * 48, 8, LANES),
            (1, E_NEW),
        ],
        [VMEM] * 7,
        [
            pltpu.VMEM((640, elements), BF),
            pltpu.VMEM((16, 8 * LANES), BF),
            pltpu.VMEM((5, 64, LANES), F32),
            pltpu.VMEM((3 * 48, 8, LANES), F32),
            pltpu.VMEM((2, 8 * LANES, LANES), F32),
        ],
        "own",
    )(first, second, counts, received[0], received[1], jac, flags)
    (state,) = call(
        edge_kernel,
        [(5, 64, E_NEW)],
        [VMEM] * 7,
        [
            pltpu.VMEM((640, 4 * LANES), BF),
            pltpu.VMEM((25, 64, LANES), F32),
            pltpu.VMEM((5, 64, E_NEW), F32),
            pltpu.SemaphoreType.DMA((5,)),
        ],
        "edge",
        HBM,
    )(from_b, from_a, *kept)
    return state, new_jac.reshape(E_NEW)


def solution(mesh):
    return jax.shard_map(
        shards,
        mesh=mesh,
        in_specs=(
            P(None, None, "curve"),
            P("curve"),
            P(),
            P("curve"),
            P("curve"),
            P(None, "curve"),
        ),
        out_specs=(P(None, None, "curve"), P("curve")),
        check_vma=False,
    )
```

```python
import math

import jax
import jax.numpy as jnp
import numpy as np
from jax import lax
from jax.experimental import pallas as pl
from jax.experimental.pallas import tpu as pltpu
from jax.sharding import PartitionSpec as P

E_NEW = 960
TIME_STEP = 0.02
OFFSETS = (-2, -1, 1, 2)
LANES = 128
BF = jnp.bfloat16
F32 = jnp.float32


def lagrange_at(points, targets):
    values_at = np.ones((len(targets), 4))
    for basis_id in range(4):
        for partner in range(4):
            if partner != basis_id:
                values_at[:, basis_id] *= (targets - points[partner]) / (
                    points[basis_id] - points[partner]
                )
    return values_at


def modes_table(points):
    return np.linalg.inv(np.polynomial.legendre.legvander(points, 3))


def node_constants():
    root = 1.0 / math.sqrt(5.0)
    points = np.array([-1.0, -root, root, 1.0])
    deriv = np.zeros((4, 4))
    bary = np.array([1.0 / np.prod([points[r] - points[c] for c in range(4) if c != r]) for r in range(4)])
    for r in range(4):
        for c in range(4):
            if r != c:
                deriv[r, c] = bary[c] / bary[r] / (points[r] - points[c])
        deriv[r, r] = -np.sum(deriv[r])
    sides = (lagrange_at(points, (points - 1.0) / 2.0), lagrange_at(points, (points + 1.0) / 2.0))
    return deriv, modes_table(points), sides


DERIV, MODES, SIDES = node_constants()
INV_W = (6.0, 1.2, 1.2, 6.0)
SELF_SURFACE = (-3.0, 0.0, 0.0, 3.0)


def low_half(shape=(8, LANES)):
    return lax.broadcasted_iota(jnp.int32, shape, 0) < 4


def swap_halves(x):
    return pltpu.roll(x, 4, axis=0)


def position():
    me = lax.axis_index("curve")
    return me, me % 2 == 0, (me // 2) % 2 == 0


def pick(flag, yes, no):
    return jnp.where(flag, yes, no)


def trace_of(ref, t, face):
    dim, side = face // 2, face % 2
    if dim == 0:
        return ref[t, pl.ds(3 * side, 16, stride=4), :]
    if dim == 2:
        return ref[t, 48 * side : 48 * side + 16, :]
    low = low_half()
    tiles = [ref[t, 16 * k + 8 * side : 16 * k + 8 * side + 8, :] for k in range(4)]
    halves = []
    for k in (0, 2):
        if side == 0:
            halves.append(jnp.where(low, tiles[k], swap_halves(tiles[k + 1])))
        else:
            halves.append(jnp.where(low, swap_halves(tiles[k]), tiles[k + 1]))
    return jnp.concatenate(halves, axis=0)


def add_to_face(ref, first, face, value):
    dim, side = face // 2, face % 2
    if dim == 0:
        where_at = (pl.ds(first + 3 * side, 16, stride=4), slice(None))
        ref[where_at] = ref[where_at] + value
    elif dim == 2:
        where_at = (slice(first + 48 * side, first + 48 * side + 16), slice(None))
        ref[where_at] = ref[where_at] + value
    else:
        low = low_half()
        keep = low if side == 0 else jnp.logical_not(low)
        for k in range(4):
            half = value[8 * (k // 2) : 8 * (k // 2) + 8, :]
            if (k % 2) != side:
                half = swap_halves(half)
            where_at = (slice(first + 16 * k + 8 * side, first + 16 * k + 8 * side + 8), slice(None))
            ref[where_at] = ref[where_at] + jnp.where(keep, half, 0.0)


def split_two(x):
    high = x.astype(BF)
    return high, (x - high.astype(F32)).astype(BF)


def one_hot(row, count, used=None, block=1):
    lanes = row.shape[1]
    packed = jnp.broadcast_to(row, (16, lanes)).astype(jnp.int16)
    ids = lax.broadcasted_iota(jnp.int32, (16, lanes), 0).astype(jnp.int16)
    one, zero = jnp.ones((16, lanes), BF), jnp.zeros((16, lanes), BF)
    pieces = []
    for first in range(0, count, 16):
        if used is not None and first % block >= used:
            pieces.append(zero)
        else:
            pieces.append(jnp.where(packed == ids + jnp.int16(first), one, zero))
    return jnp.concatenate(pieces, axis=0)


def dot32(a, b):
    return jnp.dot(a, b, preferred_element_type=F32)


def send_kernel(u_hbm, idx_hbm, jac_hbm, flag_hbm, fs_hbm, sp_hbm, modes_hbm, *rest):
    outs = rest[:4]
    slab_ref, jac_ref, flag_ref, fs_ref, speed_ref, modes_ref = rest[4:10]
    lhs, gathered, faces, idx_ref, flag_raw, sp_ref, sems = rest[10:]
    elements = u_hbm.shape[2]
    groups = elements // LANES
    loads = [pltpu.make_async_copy(idx_hbm, idx_ref, sems.at[0])]
    for g in range(groups):
        for v in range(5):
            loads.append(
                pltpu.make_async_copy(
                    u_hbm.at[v, :, pl.ds(g * LANES, LANES)], slab_ref.at[g * 5 + v], sems.at[len(loads)]
                )
            )
    for src, dst in (
        (jac_hbm, jac_ref),
        (flag_hbm, flag_raw),
        (fs_hbm, fs_ref),
        (sp_hbm, sp_ref),
        (modes_hbm, modes_ref),
    ):
        loads.append(pltpu.make_async_copy(src, dst, sems.at[len(loads)]))
    for load in loads:
        load.start()
    loads[0].wait()
    slots = idx_ref.shape[0] * LANES // 4
    row = jnp.concatenate([idx_ref[r : r + 1, :] for r in range(idx_ref.shape[0])], axis=1)
    row = jnp.broadcast_to(row, (8, 4 * slots))
    row = jnp.concatenate([row, jnp.zeros((8, 512 - 4 * slots), jnp.int32)], axis=1)
    blocks = [row[:, :LANES]]
    for b in range(1, 4):
        blocks.append(pltpu.roll(row, 512 - slots * b, axis=1)[:, :LANES])
    idx = jnp.concatenate(blocks, axis=1)
    face = jnp.zeros_like(idx)
    for f in range(1, 6):
        face = face + (idx >= f * elements).astype(jnp.int32)
    elem = idx - face * elements
    wanted = one_hot(elem[0:1], elements)
    for g in range(groups):
        for v in range(5):
            loads[1 + g * 5 + v].wait()
            high, low = split_two(slab_ref[g * 5 + v])
            lanes = slice(g * LANES, (g + 1) * LANES)
            lhs[v * 64 : (v + 1) * 64, lanes] = high
            lhs[320 + v * 64 : 320 + (v + 1) * 64, lanes] = low
    picked = dot32(lhs[...], wanted)
    for b in range(4):
        part = picked[:320, b * LANES : (b + 1) * LANES] + picked[320:, b * LANES : (b + 1) * LANES]
        gathered[b * 5 : (b + 1) * 5] = part.reshape(5, 64, LANES)
    for load in loads[1 + 5 * groups :]:
        load.wait()
    flags = flag_raw[...].astype(F32)
    flag_ref[...] = flags
    count = elements + 7.0 * jnp.sum(flags)
    rows = lax.broadcasted_iota(jnp.int32, (8, LANES), 0)
    for b in range(4):
        faces[b] = jnp.broadcast_to(face[0:1, b * LANES : (b + 1) * LANES], (16, LANES))
    me, even, even_chip = position()
    sent = (pick(even, 2, 1), pick(even, 1, 2), pick(even_chip, 3, 0), pick(even_chip, 0, 3))
    for q, b in enumerate(sent):
        fb = faces[b]
        for v in range(5):
            value = trace_of(gathered, b * 5 + v, 0)
            for f in range(1, 6):
                value = jnp.where(fb == f, trace_of(gathered, b * 5 + v, f), value)
            outs[q][v * 16 : (v + 1) * 16, :] = value
        last = b >= 2
        meta = jnp.full((8, LANES), count, F32)
        for r in range(2):
            far = groups - 2 + r
            meta = jnp.where(rows == r, pick(last, jac_ref[far : far + 1, :], jac_ref[r : r + 1, :]), meta)
            meta = jnp.where(rows == 2 + r, pick(last, flags[far : far + 1, :], flags[r : r + 1, :]), meta)
        outs[q][80:88, :] = meta
    for d in range(3):
        for v in range(5):
            speed_ref[d * 5 + v] = jnp.broadcast_to(sp_ref[d : d + 1, v : v + 1], (16, LANES))


def line_rates(x, speed, blend):
    square = [x[m] * x[m] for m in range(4)]
    prod = {}
    for m in range(4):
        for n in range(m + 1, 4):
            prod[m, n] = x[m] * x[n]
    half_speed = 0.5 * jnp.abs(speed)
    flux = []
    for m in range(3):
        central = square[m] + prod[m, m + 1] + square[m + 1]
        reach = jnp.maximum(jnp.abs(x[m]), jnp.abs(x[m + 1]))
        flux.append((speed / 6.0) * central - half_speed * reach * (x[m + 1] - x[m]))
    out = []
    for n in range(4):
        high = None
        diag = -2.0 * DERIV[n, n] / 3.0 + SELF_SURFACE[n]
        for m in range(4):
            if m != n:
                pair = prod[min(m, n), max(m, n)] + square[m]
                term = float(-DERIV[n, m] / 3.0) * pair
                high = term if high is None else high + term
        if n in (0, 3):
            high = high + float(diag) * square[n]
        high = speed * high
        if n == 0:
            low = -INV_W[0] * flux[0]
        elif n == 3:
            low = INV_W[3] * flux[2]
        else:
            low = INV_W[n] * (flux[n - 1] - flux[n])
        out.append(high + blend * (low - high))
    return out


def local_kernel(slab_ref, jac_ref, sp_ref, modes_ref, fs_ref, base_ref, out_ref, first, rows_s, lhs):
    groups = jac_ref.shape[0]
    outside_traces(slab_ref, fs_ref, out_ref, lhs)
    for g in range(groups):
        first[:, g * LANES : (g + 1) * LANES] = slab_ref[g * 5]
    modal = jnp.dot(
        modes_ref[:, :64], first[...], precision=lax.Precision.HIGHEST, preferred_element_type=F32
    )
    energy = modal * modal
    top = jnp.sum(energy * modes_ref[:, 64:65], axis=0, keepdims=True)
    whole = jnp.sum(energy, axis=0, keepdims=True)
    ratio = top / (whole + 1e-06)
    blend_all = 0.5 * ratio / (ratio + 0.1)
    for g in range(groups):
        rows_s[g] = jnp.broadcast_to(blend_all[:, g * LANES : (g + 1) * LANES], (8, LANES))
        rows_s[groups + g] = jnp.broadcast_to(jac_ref[g : g + 1, :] * TIME_STEP, (8, LANES))

    def one(t, carry):
        g = t // 5
        v = t - 5 * g
        blend = rows_s[g]
        scale = rows_s[groups + g]
        low = low_half()
        speeds = [sp_ref[5 * d + v, 0:8, :] for d in range(3)]
        for kh in range(2):
            at = [(t, pl.ds(32 * kh + i, 8, stride=4), slice(None)) for i in range(4)]
            rate = line_rates([slab_ref[a] for a in at], speeds[0], blend)
            for i in range(4):
                base_ref[at[i]] = rate[i]
        tile = [[slab_ref[t, 16 * k + 8 * h : 16 * k + 8 * h + 8, :] for h in range(2)] for k in range(4)]
        rates = [[None, None] for _ in range(4)]
        for h in range(2):
            r = line_rates([tile[k][h] for k in range(4)], speeds[2], blend)
            for k in range(4):
                rates[k][h] = r[k]
        for k in (0, 2):
            x = []
            for h in range(2):
                x.append(jnp.where(low, tile[k][h], swap_halves(tile[k + 1][h])))
                x.append(jnp.where(low, swap_halves(tile[k][h]), tile[k + 1][h]))
            r = line_rates(x, speeds[1], blend)
            for h in range(2):
                one_row, two_row = r[2 * h], r[2 * h + 1]
                rates[k][h] = rates[k][h] + jnp.where(low, one_row, swap_halves(two_row))
                rates[k + 1][h] = rates[k + 1][h] + jnp.where(low, swap_halves(one_row), two_row)
        for k in range(4):
            for h in range(2):
                at = (t, slice(16 * k + 8 * h, 16 * k + 8 * h + 8), slice(None))
                base_ref[at] = tile[k][h] + scale * (rates[k][h] + base_ref[at])
        return carry

    lax.fori_loop(0, 5 * groups, one, 0)


def outside_traces(slab_ref, fs_ref, out_ref, lhs):
    elements = fs_ref.shape[1]
    groups = elements // LANES
    for f in range(6):
        partner = f + 1 - 2 * (f % 2)
        for g in range(groups):
            for v in range(5):
                high, low = split_two(trace_of(slab_ref, g * 5 + v, partner))
                lhs[v * 16 : (v + 1) * 16, g * LANES : (g + 1) * LANES] = high
                lhs[80 + v * 16 : 80 + (v + 1) * 16, g * LANES : (g + 1) * LANES] = low
        picked = dot32(lhs[...], one_hot(fs_ref[f : f + 1, :] - partner * elements, elements))
        near = fs_ref[f : f + 1, :] < 6 * elements
        value = jnp.where(near, picked[:80] + picked[80:], 0.0)
        for g in range(groups):
            out_ref[f * groups + g] = value[:, g * LANES : (g + 1) * LANES]


def add_ghosts(out_ref, fs_ref, rd, rb, rc, ra, full_ref, lhs):
    elements = fs_ref.shape[1]
    groups = elements // LANES
    slots = 96
    me, even, even_chip = position()
    spots = (pick(even, 2, 1), pick(even, 1, 2), pick(even_chip, 3, 0), pick(even_chip, 0, 3))
    for spot, ref in zip(spots, (ra, rb, rc, rd)):
        high, low = split_two(ref[0:80, :])
        lanes = pl.ds(pl.multiple_of(spot * LANES, LANES), LANES)
        lhs[0:80, lanes] = high
        lhs[80:160, lanes] = low
    for f in range(6):
        ghost = fs_ref[f : f + 1, :] - 6 * elements
        place = jnp.zeros_like(ghost)
        for b in range(1, 4):
            place = place + (ghost >= b * slots).astype(jnp.int32)
        column = ghost + place * (LANES - slots)
        picked = dot32(lhs[...], one_hot(column, 4 * LANES, slots, LANES))
        picked = picked[:80] + picked[80:]
        for g in range(groups):
            full_ref[f * groups + g] = out_ref[f * groups + g] + picked[:, g * LANES : (g + 1) * LANES]


def refine_tables(ra, rb, jac_ref, flag_ref, meta_ref, cols_ref):
    _, even, _ = position()
    near_a, near_b = ra[80:88, :], rb[80:88, :]
    below, above = pick(even, near_b, near_a), pick(even, near_a, near_b)
    jac = jnp.concatenate([below[0:2], jac_ref[...], above[0:2]], axis=0)
    flag = jnp.concatenate([below[2:4], flag_ref[...], above[2:4]], axis=0)
    sizes = 1.0 + 7.0 * flag
    lane0 = lax.broadcasted_iota(jnp.int32, (LANES, LANES), 0)
    lane1 = lax.broadcasted_iota(jnp.int32, (LANES, LANES), 1)
    upper = jnp.where(lane0 < lane1, 1.0, 0.0).astype(BF)
    before = dot32(sizes.astype(BF), upper)
    row_total = jnp.sum(sizes, axis=1, keepdims=True)
    running = jnp.zeros((1, 1), F32)
    starts = []
    for r in range(8):
        starts.append(running)
        running = running + row_total[r : r + 1]
    row0 = lax.broadcasted_iota(jnp.int32, (8, LANES), 0)
    for r in range(8):
        before = before + jnp.where(row0 == r, starts[r], 0.0)
    place = before - starts[2]
    ends = place + sizes
    place_hi = jnp.floor(place * (1.0 / 256.0))
    place_lo = place - 256.0 * place_hi
    jac_a = jac.astype(BF)
    jac_b = (jac - jac_a.astype(F32)).astype(BF)
    jac_c = (jac - jac_a.astype(F32) - jac_b.astype(F32)).astype(BF)
    rows16 = lax.broadcasted_iota(jnp.int32, (16, LANES), 0)
    extras = [jac_a.astype(F32), jac_b.astype(F32), jac_c.astype(F32), flag, place_hi, place_lo]
    for r in range(8):
        block = jnp.zeros((16, LANES), F32)
        for q, item in enumerate(extras):
            block = jnp.where(rows16 == q, jnp.broadcast_to(item[r : r + 1, :], (16, LANES)), block)
        at = slice(r * LANES, (r + 1) * LANES)
        meta_ref[:, at] = block.astype(BF)
        for q, item in enumerate((place, ends)):
            column = jnp.transpose(jnp.broadcast_to(item[r : r + 1, :], (LANES, LANES)))
            cols_ref[q, at, :] = column.astype(jnp.int32).astype(jnp.int16)


def face_kernel(base_ref, slab_ref, out_ref, fs_ref, jac_ref, sp_ref, flag_ref, rd, rb, rc, ra, *rest):
    first_ref, second_ref, counts_ref, meta_ref, cols_ref, scales, full_ref, lhs = rest
    refine_tables(ra, rb, jac_ref, flag_ref, meta_ref, cols_ref)
    add_ghosts(out_ref, fs_ref, rd, rb, rc, ra, full_ref, lhs)
    groups = jac_ref.shape[0]
    half = groups // 2
    me, even, _ = position()
    for g in range(groups):
        scales[g] = jnp.broadcast_to(jac_ref[g : g + 1, :] * TIME_STEP, (16, LANES))
    for ref, start in ((first_ref, pick(even, half, 0)), (second_ref, pick(even, 0, half))):
        for i in range(half):
            g = start + i
            scale = scales[g]
            for v in range(5):
                t = g * 5 + v
                row = (i * 5 + v) * 64
                ref[row : row + 64, :] = base_ref[t]
                for f in range(6):
                    speed = sp_ref[5 * (f // 2) + v]
                    inner = trace_of(slab_ref, t, f)
                    outer = full_ref[f * groups + g, v * 16 : (v + 1) * 16, :]
                    central = inner * inner + inner * outer + outer * outer
                    reach = (3.0 * jnp.abs(speed)) * jnp.maximum(jnp.abs(inner), jnp.abs(outer))
                    sign = 1.0 if f % 2 == 0 else -1.0
                    value = (sign * speed) * central - reach * (inner - outer)
                    add_to_face(ref, row, f, scale * value)
    counts_ref[...] = jnp.full(counts_ref.shape, groups * LANES + 7.0 * jnp.sum(flag_ref[...]), F32)


EDGE_GROUPS = (0, 1, 5, 6, 7)
SPANS = ((0, 768), (256, 768), (256, 1024), (256, 1024))


def interpolate(res, v, coef, first, store):
    def apply(d, x):
        out = []
        for i in range(4):
            acc = coef[first + 16 * d + 4 * i] * x[0]
            for m in range(1, 4):
                acc = acc + coef[first + 16 * d + 4 * i + m] * x[m]
            out.append(acc)
        return out

    low = low_half()
    for kh in range(2):
        at = [(v, pl.ds(32 * kh + i, 8, stride=4), slice(None)) for i in range(4)]
        y = apply(0, [res[a] for a in at])
        for i in range(4):
            res[at[i]] = y[i]
    tile = [[res[v, 16 * k + 8 * q : 16 * k + 8 * q + 8, :] for q in range(2)] for k in range(4)]
    for q in range(2):
        y = apply(2, [tile[k][q] for k in range(4)])
        for k in range(4):
            tile[k][q] = y[k]
    for k in (0, 2):
        x = []
        for q in range(2):
            x.append(jnp.where(low, tile[k][q], swap_halves(tile[k + 1][q])))
            x.append(jnp.where(low, swap_halves(tile[k][q]), tile[k + 1][q]))
        y = apply(1, x)
        for q in range(2):
            one_row, two_row = y[2 * q], y[2 * q + 1]
            store(16 * k + 8 * q, jnp.where(low, one_row, swap_halves(two_row)))
            store(16 * (k + 1) + 8 * q, jnp.where(low, swap_halves(one_row), two_row))


def own_kernel(first_ref, second_ref, counts_ref, meta, cols, *rest):
    mid_ref, part_ref, low_hot, up_hot, coef_out, jout_ref = rest[:6]
    lhs, res, coef_mid = rest[6:]
    me, even, _ = position()
    for ref, start in ((first_ref, pick(even, 2, 0)), (second_ref, pick(even, 0, 2))):
        for g in range(2):
            high, low = split_two(ref[320 * g : 320 * g + 320, :])
            at = pl.ds(pl.multiple_of((start + g) * LANES, LANES), LANES)
            lhs[0:320, at] = high
            lhs[320:640, at] = low
    counts = counts_ref[...]
    half = counts.shape[0]
    upper = me >= half
    earlier = lax.broadcasted_iota(jnp.int32, counts.shape, 0) < me % half
    begin = jnp.sum(jnp.where(earlier, counts, 0.0), axis=0, keepdims=True)
    rest = float(2 * half * E_NEW) - jnp.sum(counts, axis=0, keepdims=True)
    begin = begin + pick(upper, rest, jnp.zeros_like(rest))
    begin = begin - (me * E_NEW).astype(F32)
    slots = [
        (lax.broadcasted_iota(jnp.int32, (16, LANES), 1) + g * LANES).astype(F32) - begin for g in range(8)
    ]

    for pair, (k0, k1) in enumerate(SPANS):
        pieces = []
        one, zero = jnp.ones((16, LANES), BF), jnp.zeros((16, LANES), BF)
        for h in range(2):
            slot = slots[2 * pair + h].astype(jnp.int32).astype(jnp.int16)
            column = []
            for k in range(k0, k1, 16):
                hit = jnp.logical_and(slot >= cols[0, k : k + 16, :], slot < cols[1, k : k + 16, :])
                column.append(jnp.where(hit, one, zero))
            pieces.append(jnp.concatenate(column, axis=0))
        hot = jnp.concatenate(pieces, axis=1)
        if pair == 0:
            low_hot[...] = hot[0:256]
        elif pair == 2:
            up_hot[:, 0:LANES] = hot[512:768, LANES : 2 * LANES]
        elif pair == 3:
            up_hot[:, LANES : 3 * LANES] = hot[512:768]
        picked = dot32(lhs[...], hot[256 - k0 : 768 - k0])
        known = dot32(meta[:, k0:k1], hot)
        for h in range(2):
            g = 2 * pair + h
            lanes = slice(h * LANES, (h + 1) * LANES)
            width_at = min(LANES, E_NEW - g * LANES)
            extra = known[:, lanes]
            jac_new = (extra[0:1] + extra[1:2] + extra[2:3]) * (1.0 + extra[3:4])
            jout_ref[0:1, g * LANES : g * LANES + width_at] = jac_new[:, :width_at]
            fl = jnp.broadcast_to(extra[3:4], (8, LANES))
            child = slots[g][0:8] - (256.0 * extra[4:5] + extra[5:6])
            bit2 = jnp.where(child >= 4.0, 1.0, 0.0)
            child = child - 4.0 * bit2
            bit1 = jnp.where(child >= 2.0, 1.0, 0.0)
            bit0 = child - 2.0 * bit1
            edge = g in EDGE_GROUPS
            coef, first = (coef_out, 48 * EDGE_GROUPS.index(g)) if edge else (coef_mid, 48 * (g - 2))
            for d, bit in enumerate((bit0, bit1, bit2)):
                both = fl * bit
                for i in range(4):
                    for m in range(4):
                        eye = 1.0 if i == m else 0.0
                        c = fl * float(SIDES[0][i, m] - eye) + both * float(SIDES[1][i, m] - SIDES[0][i, m]) + eye
                        coef[first + 16 * d + 4 * i + m] = c
            value = (picked[0:320, lanes] + picked[320:640, lanes]).reshape(5, 64, LANES)
            if edge:
                q = EDGE_GROUPS.index(g)
                part_ref[5 * q : 5 * q + 5] = value
            else:
                res[...] = value

                def one(v, carry, g=g, first=first):
                    def store(row, x):
                        mid_ref[5 * (g - 2) + v, row : row + 8, :] = x

                    interpolate(res, v, coef_mid, first, store)
                    return carry

                lax.fori_loop(0, 5, one, 0)


def edge_kernel(b_ref, a_ref, mid_ref, part_ref, low_hot, up_hot, coef_ref, jac_ref, out_hbm, jac_hbm, *rest):
    lhs, res, out, sems = rest
    jac_out = pltpu.make_async_copy(jac_ref, jac_hbm, sems.at[5])
    jac_out.start()
    _, even, _ = position()
    for ref, start in ((a_ref, pick(even, 2, 0)), (b_ref, pick(even, 0, 2))):
        for g in range(2):
            high, low = split_two(ref[320 * g : 320 * g + 320, :])
            at = pl.ds(pl.multiple_of((start + g) * LANES, LANES), LANES)
            lhs[0:320, at] = high
            lhs[320:640, at] = low
    picked = (dot32(lhs[:, 0:256], low_hot[...]), dot32(lhs[:, 256:512], up_hot[...]))
    for q, g in enumerate(EDGE_GROUPS):
        from_up = int(g >= 5)
        at = (g - 5 * from_up) * LANES
        value = picked[from_up][0:320, at : at + LANES] + picked[from_up][320:640, at : at + LANES]
        res[5 * q : 5 * q + 5] = part_ref[5 * q : 5 * q + 5] + value.reshape(5, 64, LANES)
    for v in range(5):
        for g in (2, 3, 4):
            out[v, :, g * LANES : (g + 1) * LANES] = mid_ref[5 * (g - 2) + v]
        for q, g in enumerate(EDGE_GROUPS):
            width_at = min(LANES, E_NEW - g * LANES)

            def store(row, x, v=v, g=g, width_at=width_at):
                out[v, row : row + 8, g * LANES : g * LANES + width_at] = x[:, :width_at]

            interpolate(res, 5 * q + v, coef_ref, 48 * q, store)
        pltpu.make_async_copy(out.at[v], out_hbm.at[v], sems.at[v]).start()
    for v in range(5):
        pltpu.make_async_copy(out.at[v], out_hbm.at[v], sems.at[v]).wait()
    jac_out.wait()


VMEM = pl.BlockSpec(memory_space=pltpu.MemorySpace.VMEM)
HBM = pl.BlockSpec(memory_space=pltpu.MemorySpace.HBM)


def swap(x, pairs):
    return lax.ppermute(x, "curve", list(pairs) + [(b, a) for a, b in pairs])


def in_hbm(x):
    return pltpu.with_memory_space_constraint(x, pltpu.MemorySpace.HBM)


def call(body, outs, specs, scratch, name, out_spec=VMEM, flops=100_000_000):
    shapes = []
    for item in outs:
        shape, dtype = item if isinstance(item[0], tuple) else (item, F32)
        shapes.append(jax.ShapeDtypeStruct(shape, dtype))
    return pl.pallas_call(
        body,
        out_shape=tuple(shapes),
        in_specs=specs,
        out_specs=tuple(out_spec for _ in outs),
        scratch_shapes=scratch,
        name=name,
        compiler_params=pltpu.CompilerParams(vmem_limit_bytes=16 << 20),
    )


def shards(nodal_state, inverse_jacobian, speeds, refine_flags, send_index, face_source):
    elements = nodal_state.shape[2]
    groups = elements // LANES
    total = lax.axis_size("curve")
    half = total // 2
    idx = send_index.reshape(-1, LANES)
    jac = inverse_jacobian.reshape(groups, LANES)
    flags = refine_flags.reshape(groups, LANES)
    degrees = np.arange(4)
    top = (np.maximum(np.maximum(degrees[:, None, None], degrees[None, :, None]), degrees) == 3).reshape(64, 1)
    kron = np.kron(MODES, np.kron(MODES, MODES))
    modes = jnp.asarray(np.concatenate([kron, np.repeat(top, 64, axis=1)], axis=1), F32)
    slabs = 5 * groups

    outs = call(
        send_kernel,
        [(88, LANES)] * 4
        + [
            (slabs, 64, LANES),
            (groups, LANES),
            (groups, LANES),
            ((6, elements), jnp.int32),
            (15, 16, LANES),
            (64, LANES),
        ],
        [HBM] * 7,
        [
            pltpu.VMEM((640, elements), BF),
            pltpu.VMEM((20, 64, LANES), F32),
            pltpu.VMEM((4, 16, LANES), jnp.int32),
            pltpu.VMEM(idx.shape, jnp.int32),
            pltpu.VMEM((groups, LANES), jnp.int32),
            pltpu.VMEM(speeds.shape, F32),
            pltpu.SemaphoreType.DMA((slabs + 6,)),
        ],
        "send",
    )(*(in_hbm(x) for x in (nodal_state, idx, jac, flags, face_source, speeds, modes)))
    sends = outs[:4]
    slab, jac, flags, face_source, speeds, modes = outs[4:]
    pair_a = [(i, i + 1) for i in range(0, total, 2)]
    pair_b = [(i, (i + 1) % total) for i in range(1, total, 2)]
    pair_c = [(i, i + 2) for i in range(total) if (i // 2) % 2 == 0]
    pair_d = [(i, (i + 2) % total) for i in range(total) if (i // 2) % 2 == 1]
    received = [swap(x, pairs) for x, pairs in zip(sends, (pair_a, pair_b, pair_c, pair_d))]

    base, outside = call(
        local_kernel,
        [(slabs, 64, LANES), (6 * groups, 80, LANES)],
        [VMEM] * 5,
        [
            pltpu.VMEM((64, elements), F32),
            pltpu.VMEM((2 * groups, 8, LANES), F32),
            pltpu.VMEM((160, elements), BF),
        ],
        "local",
    )(slab, jac, speeds, modes, face_source)
    rows = slabs // 2 * 64
    first, second, counts, meta, cols = call(
        face_kernel,
        [
            (rows, LANES),
            (rows, LANES),
            (half, LANES),
            ((16, 8 * LANES), BF),
            ((2, 8 * LANES, LANES), jnp.int16),
        ],
        [VMEM] * 11,
        [
            pltpu.VMEM((groups, 16, LANES), F32),
            pltpu.VMEM((6 * groups, 80, LANES), F32),
            pltpu.VMEM((160, 4 * LANES), BF),
        ],
        "faces",
    )(base, slab, outside, face_source, jac, speeds, flags, *(received[q] for q in (3, 1, 2, 0)))

    from_a = swap(first, pair_a)
    from_b = swap(second, pair_b[:-1])

    halves = [list(range(half)), list(range(half, total))]
    counts = lax.all_to_all(counts, "curve", 0, 0, axis_index_groups=halves, tiled=True)

    kept = call(
        own_kernel,
        [
            (15, 64, LANES),
            (25, 64, LANES),
            ((256, 256), BF),
            ((256, 384), BF),
            (5 * 48, 8, LANES),
            (1, E_NEW),
        ],
        [VMEM] * 5,
        [
            pltpu.VMEM((640, elements), BF),
            pltpu.VMEM((5, 64, LANES), F32),
            pltpu.VMEM((3 * 48, 8, LANES), F32),
        ],
        "own",
    )(first, second, counts, meta, cols)
    state, new_jac = call(
        edge_kernel,
        [(5, 64, E_NEW), (1, E_NEW)],
        [VMEM] * 8,
        [
            pltpu.VMEM((640, 4 * LANES), BF),
            pltpu.VMEM((25, 64, LANES), F32),
            pltpu.VMEM((5, 64, E_NEW), F32),
            pltpu.SemaphoreType.DMA((6,)),
        ],
        "edge",
        HBM,
    )(from_b, from_a, *kept)
    return state, new_jac.reshape(E_NEW)


def solution(mesh):
    return jax.shard_map(
        shards,
        mesh=mesh,
        in_specs=(
            P(None, None, "curve"),
            P("curve"),
            P(),
            P("curve"),
            P("curve"),
            P(None, "curve"),
        ),
        out_specs=(P(None, None, "curve"), P("curve")),
        check_vma=False,
    )
```

```python
import math

import jax
import jax.numpy as jnp
import numpy as np
from jax import lax
from jax.experimental import pallas as pl
from jax.experimental.pallas import tpu as pltpu
from jax.sharding import PartitionSpec as P

E_NEW = 960
TIME_STEP = 0.02
OFFSETS = (-2, -1, 1, 2)
LANES = 128
BF = jnp.bfloat16
F32 = jnp.float32


def lagrange_at(points, targets):
    values_at = np.ones((len(targets), 4))
    for basis_id in range(4):
        for partner in range(4):
            if partner != basis_id:
                values_at[:, basis_id] *= (targets - points[partner]) / (
                    points[basis_id] - points[partner]
                )
    return values_at


def modes_table(points):
    return np.linalg.inv(np.polynomial.legendre.legvander(points, 3))


def node_constants():
    root = 1.0 / math.sqrt(5.0)
    points = np.array([-1.0, -root, root, 1.0])
    deriv = np.zeros((4, 4))
    bary = np.array([1.0 / np.prod([points[r] - points[c] for c in range(4) if c != r]) for r in range(4)])
    for r in range(4):
        for c in range(4):
            if r != c:
                deriv[r, c] = bary[c] / bary[r] / (points[r] - points[c])
        deriv[r, r] = -np.sum(deriv[r])
    sides = (lagrange_at(points, (points - 1.0) / 2.0), lagrange_at(points, (points + 1.0) / 2.0))
    return deriv, modes_table(points), sides


DERIV, MODES, SIDES = node_constants()
INV_W = (6.0, 1.2, 1.2, 6.0)
SELF_SURFACE = (-3.0, 0.0, 0.0, 3.0)


def low_half(shape=(8, LANES)):
    return lax.broadcasted_iota(jnp.int32, shape, 0) < 4


def swap_halves(x):
    return pltpu.roll(x, 4, axis=0)


def position():
    me = lax.axis_index("curve")
    return me, me % 2 == 0, (me // 2) % 2 == 0


def pick(flag, yes, no):
    return jnp.where(flag, yes, no)


def trace_of(ref, t, face):
    dim, side = face // 2, face % 2
    if dim == 0:
        return ref[t, pl.ds(3 * side, 16, stride=4), :]
    if dim == 2:
        return ref[t, 48 * side : 48 * side + 16, :]
    low = low_half()
    tiles = [ref[t, 16 * k + 8 * side : 16 * k + 8 * side + 8, :] for k in range(4)]
    halves = []
    for k in (0, 2):
        if side == 0:
            halves.append(jnp.where(low, tiles[k], swap_halves(tiles[k + 1])))
        else:
            halves.append(jnp.where(low, swap_halves(tiles[k]), tiles[k + 1]))
    return jnp.concatenate(halves, axis=0)


def add_to_face(ref, first, face, value):
    dim, side = face // 2, face % 2
    if dim == 0:
        where_at = (pl.ds(first + 3 * side, 16, stride=4), slice(None))
        ref[where_at] = ref[where_at] + value
    elif dim == 2:
        where_at = (slice(first + 48 * side, first + 48 * side + 16), slice(None))
        ref[where_at] = ref[where_at] + value
    else:
        low = low_half()
        keep = low if side == 0 else jnp.logical_not(low)
        for k in range(4):
            half = value[8 * (k // 2) : 8 * (k // 2) + 8, :]
            if (k % 2) != side:
                half = swap_halves(half)
            where_at = (slice(first + 16 * k + 8 * side, first + 16 * k + 8 * side + 8), slice(None))
            ref[where_at] = ref[where_at] + jnp.where(keep, half, 0.0)


def split_two(x):
    high = x.astype(BF)
    return high, (x - high.astype(F32)).astype(BF)


def one_hot(row, count, used=None, block=1):
    lanes = row.shape[1]
    packed = jnp.broadcast_to(row, (16, lanes)).astype(jnp.int16)
    ids = lax.broadcasted_iota(jnp.int32, (16, lanes), 0).astype(jnp.int16)
    one, zero = jnp.ones((16, lanes), BF), jnp.zeros((16, lanes), BF)
    pieces = []
    for first in range(0, count, 16):
        if used is not None and first % block >= used:
            pieces.append(zero)
        else:
            pieces.append(jnp.where(packed == ids + jnp.int16(first), one, zero))
    return jnp.concatenate(pieces, axis=0)


def dot32(a, b):
    return jnp.dot(a, b, preferred_element_type=F32)


def send_kernel(u_hbm, idx_hbm, jac_hbm, flag_hbm, fs_hbm, sp_hbm, modes_hbm, *rest):
    outs = rest[:4]
    slab_ref, jac_ref, flag_ref, fs_ref, speed_ref, modes_ref = rest[4:10]
    lhs, gathered, faces, idx_ref, flag_raw, sp_ref, sems = rest[10:]
    elements = u_hbm.shape[2]
    groups = elements // LANES
    loads = [pltpu.make_async_copy(idx_hbm, idx_ref, sems.at[0])]
    for g in range(groups):
        for v in range(5):
            loads.append(
                pltpu.make_async_copy(
                    u_hbm.at[v, :, pl.ds(g * LANES, LANES)], slab_ref.at[g * 5 + v], sems.at[len(loads)]
                )
            )
    for src, dst in (
        (jac_hbm, jac_ref),
        (flag_hbm, flag_raw),
        (fs_hbm, fs_ref),
        (sp_hbm, sp_ref),
        (modes_hbm, modes_ref),
    ):
        loads.append(pltpu.make_async_copy(src, dst, sems.at[len(loads)]))
    for load in loads:
        load.start()
    loads[0].wait()
    slots = idx_ref.shape[0] * LANES // 4
    row = jnp.concatenate([idx_ref[r : r + 1, :] for r in range(idx_ref.shape[0])], axis=1)
    row = jnp.broadcast_to(row, (8, 4 * slots))
    row = jnp.concatenate([row, jnp.zeros((8, 512 - 4 * slots), jnp.int32)], axis=1)
    blocks = [row[:, :LANES]]
    for b in range(1, 4):
        blocks.append(pltpu.roll(row, 512 - slots * b, axis=1)[:, :LANES])
    idx = jnp.concatenate(blocks, axis=1)
    face = jnp.zeros_like(idx)
    for f in range(1, 6):
        face = face + (idx >= f * elements).astype(jnp.int32)
    elem = idx - face * elements
    wanted = one_hot(elem[0:1], elements)
    for g in range(groups):
        for v in range(5):
            loads[1 + g * 5 + v].wait()
            high, low = split_two(slab_ref[g * 5 + v])
            lanes = slice(g * LANES, (g + 1) * LANES)
            lhs[v * 64 : (v + 1) * 64, lanes] = high
            lhs[320 + v * 64 : 320 + (v + 1) * 64, lanes] = low
    picked = dot32(lhs[...], wanted)
    for b in range(4):
        part = picked[:320, b * LANES : (b + 1) * LANES] + picked[320:, b * LANES : (b + 1) * LANES]
        gathered[b * 5 : (b + 1) * 5] = part.reshape(5, 64, LANES)
    for load in loads[1 + 5 * groups :]:
        load.wait()
    flags = flag_raw[...].astype(F32)
    flag_ref[...] = flags
    count = elements + 7.0 * jnp.sum(flags)
    rows = lax.broadcasted_iota(jnp.int32, (8, LANES), 0)
    for b in range(4):
        faces[b] = jnp.broadcast_to(face[0:1, b * LANES : (b + 1) * LANES], (16, LANES))
    me, even, even_chip = position()
    sent = (pick(even, 2, 1), pick(even, 1, 2), pick(even_chip, 3, 0), pick(even_chip, 0, 3))
    for q, b in enumerate(sent):
        fb = faces[b]
        for v in range(5):
            value = trace_of(gathered, b * 5 + v, 0)
            for f in range(1, 6):
                value = jnp.where(fb == f, trace_of(gathered, b * 5 + v, f), value)
            outs[q][v * 16 : (v + 1) * 16, :] = value
        last = b >= 2
        meta = jnp.full((8, LANES), count, F32)
        for r in range(2):
            far = groups - 2 + r
            meta = jnp.where(rows == r, pick(last, jac_ref[far : far + 1, :], jac_ref[r : r + 1, :]), meta)
            meta = jnp.where(rows == 2 + r, pick(last, flags[far : far + 1, :], flags[r : r + 1, :]), meta)
        outs[q][80:88, :] = meta
    for d in range(3):
        for v in range(5):
            speed_ref[d * 5 + v] = jnp.broadcast_to(sp_ref[d : d + 1, v : v + 1], (16, LANES))


def line_weights(speed, blend):
    return speed * (1.0 - blend), blend * speed * (1.0 / 6.0), blend * (0.5 * jnp.abs(speed))


def line_rates(x, weights):
    high_weight, central_weight, jump_weight = weights
    square = [x[m] * x[m] for m in range(4)]
    size = [jnp.abs(x[m]) for m in range(4)]
    prod = {}
    for m in range(4):
        for n in range(m + 1, 4):
            prod[m, n] = x[m] * x[n]
    pair = {(n, m): prod[min(m, n), max(m, n)] + square[m] for n in range(4) for m in range(4) if m != n}
    flux = []
    for m in range(3):
        central = pair[m, m + 1] + square[m]
        jump = jnp.maximum(size[m], size[m + 1]) * (x[m + 1] - x[m])
        flux.append(central_weight * central - jump_weight * jump)
    low = (
        -INV_W[0] * flux[0],
        INV_W[1] * (flux[0] - flux[1]),
        INV_W[2] * (flux[1] - flux[2]),
        INV_W[3] * flux[2],
    )
    out = []
    for n in range(4):
        high = None
        for m in range(4):
            if m != n:
                term = float(-DERIV[n, m] / 3.0) * pair[n, m]
                high = term if high is None else high + term
        if n in (0, 3):
            high = high + float(-2.0 * DERIV[n, n] / 3.0 + SELF_SURFACE[n]) * square[n]
        out.append(high_weight * high + low[n])
    return out


def local_kernel(slab_ref, jac_ref, sp_ref, modes_ref, fs_ref, base_ref, out_ref, first, rows_s, lhs):
    groups = jac_ref.shape[0]
    outside_traces(slab_ref, fs_ref, out_ref, lhs)
    for g in range(groups):
        first[:, g * LANES : (g + 1) * LANES] = slab_ref[g * 5]
    modal = jnp.dot(
        modes_ref[:, :64], first[...], precision=lax.Precision.HIGHEST, preferred_element_type=F32
    )
    energy = modal * modal
    top = jnp.sum(energy * modes_ref[:, 64:65], axis=0, keepdims=True)
    whole = jnp.sum(energy, axis=0, keepdims=True)
    ratio = top / (whole + 1e-06)
    blend_all = 0.5 * ratio / (ratio + 0.1)
    for g in range(groups):
        rows_s[g] = jnp.broadcast_to(blend_all[:, g * LANES : (g + 1) * LANES], (8, LANES))
        rows_s[groups + g] = jnp.broadcast_to(jac_ref[g : g + 1, :] * TIME_STEP, (8, LANES))

    def one(t, carry):
        g = t // 5
        v = t - 5 * g
        blend = rows_s[g]
        scale = rows_s[groups + g]
        low = low_half()
        weights = [line_weights(sp_ref[5 * d + v, 0:8, :], blend) for d in range(3)]
        for kh in range(2):
            at = [(t, pl.ds(32 * kh + i, 8, stride=4), slice(None)) for i in range(4)]
            rate = line_rates([slab_ref[a] for a in at], weights[0])
            for i in range(4):
                base_ref[at[i]] = rate[i]
        tile = [[slab_ref[t, 16 * k + 8 * h : 16 * k + 8 * h + 8, :] for h in range(2)] for k in range(4)]
        rates = [[None, None] for _ in range(4)]
        for h in range(2):
            r = line_rates([tile[k][h] for k in range(4)], weights[2])
            for k in range(4):
                rates[k][h] = r[k]
        for k in (0, 2):
            x = []
            for h in range(2):
                x.append(jnp.where(low, tile[k][h], swap_halves(tile[k + 1][h])))
                x.append(jnp.where(low, swap_halves(tile[k][h]), tile[k + 1][h]))
            r = line_rates(x, weights[1])
            for h in range(2):
                one_row, two_row = r[2 * h], r[2 * h + 1]
                rates[k][h] = rates[k][h] + jnp.where(low, one_row, swap_halves(two_row))
                rates[k + 1][h] = rates[k + 1][h] + jnp.where(low, swap_halves(one_row), two_row)
        for k in range(4):
            for h in range(2):
                at = (t, slice(16 * k + 8 * h, 16 * k + 8 * h + 8), slice(None))
                base_ref[at] = tile[k][h] + scale * (rates[k][h] + base_ref[at])
        return carry

    lax.fori_loop(0, 5 * groups, one, 0)


def outside_traces(slab_ref, fs_ref, out_ref, lhs):
    elements = fs_ref.shape[1]
    groups = elements // LANES
    for f in range(6):
        partner = f + 1 - 2 * (f % 2)
        for g in range(groups):
            for v in range(5):
                high, low = split_two(trace_of(slab_ref, g * 5 + v, partner))
                lhs[v * 16 : (v + 1) * 16, g * LANES : (g + 1) * LANES] = high
                lhs[80 + v * 16 : 80 + (v + 1) * 16, g * LANES : (g + 1) * LANES] = low
        picked = dot32(lhs[...], one_hot(fs_ref[f : f + 1, :] - partner * elements, elements))
        near = fs_ref[f : f + 1, :] < 6 * elements
        value = jnp.where(near, picked[:80] + picked[80:], 0.0)
        for g in range(groups):
            out_ref[f * groups + g] = value[:, g * LANES : (g + 1) * LANES]


def add_ghosts(out_ref, fs_ref, rd, rb, rc, ra, full_ref, lhs):
    elements = fs_ref.shape[1]
    groups = elements // LANES
    slots = 96
    me, even, even_chip = position()
    spots = (pick(even, 2, 1), pick(even, 1, 2), pick(even_chip, 3, 0), pick(even_chip, 0, 3))
    for spot, ref in zip(spots, (ra, rb, rc, rd)):
        high, low = split_two(ref[0:80, :])
        lanes = pl.ds(pl.multiple_of(spot * LANES, LANES), LANES)
        lhs[0:80, lanes] = high
        lhs[80:160, lanes] = low
    for f in range(6):
        ghost = fs_ref[f : f + 1, :] - 6 * elements
        place = jnp.zeros_like(ghost)
        for b in range(1, 4):
            place = place + (ghost >= b * slots).astype(jnp.int32)
        column = ghost + place * (LANES - slots)
        picked = dot32(lhs[...], one_hot(column, 4 * LANES, slots, LANES))
        picked = picked[:80] + picked[80:]
        for g in range(groups):
            full_ref[f * groups + g] = out_ref[f * groups + g] + picked[:, g * LANES : (g + 1) * LANES]


def refine_tables(ra, rb, jac_ref, flag_ref, meta_ref, cols_ref):
    _, even, _ = position()
    near_a, near_b = ra[80:88, :], rb[80:88, :]
    below, above = pick(even, near_b, near_a), pick(even, near_a, near_b)
    jac = jnp.concatenate([below[0:2], jac_ref[...], above[0:2]], axis=0)
    flag = jnp.concatenate([below[2:4], flag_ref[...], above[2:4]], axis=0)
    sizes = 1.0 + 7.0 * flag
    lane0 = lax.broadcasted_iota(jnp.int32, (LANES, LANES), 0)
    lane1 = lax.broadcasted_iota(jnp.int32, (LANES, LANES), 1)
    upper = jnp.where(lane0 < lane1, 1.0, 0.0).astype(BF)
    before = dot32(sizes.astype(BF), upper)
    row_total = jnp.sum(sizes, axis=1, keepdims=True)
    running = jnp.zeros((1, 1), F32)
    starts = []
    for r in range(8):
        starts.append(running)
        running = running + row_total[r : r + 1]
    row0 = lax.broadcasted_iota(jnp.int32, (8, LANES), 0)
    for r in range(8):
        before = before + jnp.where(row0 == r, starts[r], 0.0)
    place = before - starts[2]
    ends = place + sizes
    place_hi = jnp.floor(place * (1.0 / 256.0))
    place_lo = place - 256.0 * place_hi
    jac_a = jac.astype(BF)
    jac_b = (jac - jac_a.astype(F32)).astype(BF)
    jac_c = (jac - jac_a.astype(F32) - jac_b.astype(F32)).astype(BF)
    rows16 = lax.broadcasted_iota(jnp.int32, (16, LANES), 0)
    extras = [jac_a.astype(F32), jac_b.astype(F32), jac_c.astype(F32), flag, place_hi, place_lo]
    for r in range(8):
        block = jnp.zeros((16, LANES), F32)
        for q, item in enumerate(extras):
            block = jnp.where(rows16 == q, jnp.broadcast_to(item[r : r + 1, :], (16, LANES)), block)
        at = slice(r * LANES, (r + 1) * LANES)
        meta_ref[:, at] = block.astype(BF)
        for q, item in enumerate((place, ends)):
            column = jnp.transpose(jnp.broadcast_to(item[r : r + 1, :], (LANES, LANES)))
            cols_ref[q, at, :] = column.astype(jnp.int32).astype(jnp.int16)


def face_kernel(base_ref, slab_ref, out_ref, fs_ref, jac_ref, sp_ref, flag_ref, rd, rb, rc, ra, *rest):
    first_ref, second_ref, counts_ref, meta_ref, cols_ref, scales, full_ref, lhs = rest
    refine_tables(ra, rb, jac_ref, flag_ref, meta_ref, cols_ref)
    add_ghosts(out_ref, fs_ref, rd, rb, rc, ra, full_ref, lhs)
    groups = jac_ref.shape[0]
    half = groups // 2
    me, even, _ = position()
    for g in range(groups):
        scales[g] = jnp.broadcast_to(jac_ref[g : g + 1, :] * TIME_STEP, (16, LANES))
    for ref, start in ((first_ref, pick(even, half, 0)), (second_ref, pick(even, 0, half))):
        for i in range(half):
            g = start + i
            scale = scales[g]
            for v in range(5):
                t = g * 5 + v
                row = (i * 5 + v) * 64
                ref[row : row + 64, :] = base_ref[t]
                for f in range(6):
                    speed = sp_ref[5 * (f // 2) + v]
                    inner = trace_of(slab_ref, t, f)
                    outer = full_ref[f * groups + g, v * 16 : (v + 1) * 16, :]
                    central = inner * inner + inner * outer + outer * outer
                    reach = (3.0 * jnp.abs(speed)) * jnp.maximum(jnp.abs(inner), jnp.abs(outer))
                    sign = 1.0 if f % 2 == 0 else -1.0
                    value = (sign * speed) * central - reach * (inner - outer)
                    add_to_face(ref, row, f, scale * value)
    counts_ref[...] = jnp.full(counts_ref.shape, groups * LANES + 7.0 * jnp.sum(flag_ref[...]), F32)


SPANS = ((0, 768), (256, 768), (256, 1024), (256, 1024))


def interpolate(res, v, coef, first, store):
    def apply(d, x):
        out = []
        for i in range(4):
            acc = coef[first + 16 * d + 4 * i] * x[0]
            for m in range(1, 4):
                acc = acc + coef[first + 16 * d + 4 * i + m] * x[m]
            out.append(acc)
        return out

    low = low_half()
    for kh in range(2):
        at = [(v, pl.ds(32 * kh + i, 8, stride=4), slice(None)) for i in range(4)]
        y = apply(0, [res[a] for a in at])
        for i in range(4):
            res[at[i]] = y[i]
    tile = [[res[v, 16 * k + 8 * q : 16 * k + 8 * q + 8, :] for q in range(2)] for k in range(4)]
    for q in range(2):
        y = apply(2, [tile[k][q] for k in range(4)])
        for k in range(4):
            tile[k][q] = y[k]
    for k in (0, 2):
        x = []
        for q in range(2):
            x.append(jnp.where(low, tile[k][q], swap_halves(tile[k + 1][q])))
            x.append(jnp.where(low, swap_halves(tile[k][q]), tile[k + 1][q]))
        y = apply(1, x)
        for q in range(2):
            one_row, two_row = y[2 * q], y[2 * q + 1]
            store(16 * k + 8 * q, jnp.where(low, one_row, swap_halves(two_row)))
            store(16 * (k + 1) + 8 * q, jnp.where(low, swap_halves(one_row), two_row))


def refine_kernel(b_ref, a_ref, first_ref, second_ref, counts_ref, meta, cols, out_hbm, jac_hbm, *rest):
    lhs, res, coef, out, jout_ref, sems = rest
    me, even, _ = position()
    parts = (
        (first_ref, pick(even, 4, 2)),
        (second_ref, pick(even, 2, 4)),
        (b_ref, pick(even, 0, 6)),
        (a_ref, pick(even, 6, 0)),
    )
    for ref, start in parts:
        for g in range(2):
            high, low = split_two(ref[320 * g : 320 * g + 320, :])
            at = pl.ds(pl.multiple_of((start + g) * LANES, LANES), LANES)
            lhs[0:320, at] = high
            lhs[320:640, at] = low
    counts = counts_ref[...]
    half = counts.shape[0]
    upper = me >= half
    earlier = lax.broadcasted_iota(jnp.int32, counts.shape, 0) < me % half
    begin = jnp.sum(jnp.where(earlier, counts, 0.0), axis=0, keepdims=True)
    rest = float(2 * half * E_NEW) - jnp.sum(counts, axis=0, keepdims=True)
    begin = begin + pick(upper, rest, jnp.zeros_like(rest))
    begin = begin - (me * E_NEW).astype(F32)
    slots = [
        (lax.broadcasted_iota(jnp.int32, (16, LANES), 1) + g * LANES).astype(F32) - begin for g in range(8)
    ]

    for pair, (k0, k1) in enumerate(SPANS):
        pieces = []
        one, zero = jnp.ones((16, LANES), BF), jnp.zeros((16, LANES), BF)
        for h in range(2):
            slot = slots[2 * pair + h].astype(jnp.int32).astype(jnp.int16)
            column = []
            for k in range(k0, k1, 16):
                hit = jnp.logical_and(slot >= cols[0, k : k + 16, :], slot < cols[1, k : k + 16, :])
                column.append(jnp.where(hit, one, zero))
            pieces.append(jnp.concatenate(column, axis=0))
        hot = jnp.concatenate(pieces, axis=1)
        picked = dot32(lhs[:, k0:k1], hot)
        known = dot32(meta[:, k0:k1], hot)
        for h in range(2):
            g = 2 * pair + h
            lanes = slice(h * LANES, (h + 1) * LANES)
            width_at = min(LANES, E_NEW - g * LANES)
            extra = known[:, lanes]
            jac_new = (extra[0:1] + extra[1:2] + extra[2:3]) * (1.0 + extra[3:4])
            jout_ref[0:1, g * LANES : g * LANES + width_at] = jac_new[:, :width_at]
            fl = jnp.broadcast_to(extra[3:4], (8, LANES))
            child = slots[g][0:8] - (256.0 * extra[4:5] + extra[5:6])
            bit2 = jnp.where(child >= 4.0, 1.0, 0.0)
            child = child - 4.0 * bit2
            bit1 = jnp.where(child >= 2.0, 1.0, 0.0)
            bit0 = child - 2.0 * bit1
            for d, bit in enumerate((bit0, bit1, bit2)):
                both = fl * bit
                for i in range(4):
                    for m in range(4):
                        eye = 1.0 if i == m else 0.0
                        c = fl * float(SIDES[0][i, m] - eye) + both * float(SIDES[1][i, m] - SIDES[0][i, m]) + eye
                        coef[48 * g + 16 * d + 4 * i + m] = c
            res[5 * g : 5 * g + 5] = (picked[0:320, lanes] + picked[320:640, lanes]).reshape(5, 64, LANES)
    copies = [pltpu.make_async_copy(jout_ref, jac_hbm, sems.at[5])]
    copies[0].start()
    for v in range(5):
        for g in range(8):
            width_at = min(LANES, E_NEW - g * LANES)

            def store(row, x, v=v, g=g, width_at=width_at):
                out[v, row : row + 8, g * LANES : g * LANES + width_at] = x[:, :width_at]

            interpolate(res, 5 * g + v, coef, 48 * g, store)
        copies.append(pltpu.make_async_copy(out.at[v], out_hbm.at[v], sems.at[v]))
        copies[-1].start()
    for copy in copies:
        copy.wait()


VMEM = pl.BlockSpec(memory_space=pltpu.MemorySpace.VMEM)
HBM = pl.BlockSpec(memory_space=pltpu.MemorySpace.HBM)


def swap(x, pairs):
    return lax.ppermute(x, "curve", list(pairs) + [(b, a) for a, b in pairs])


def in_hbm(x):
    return pltpu.with_memory_space_constraint(x, pltpu.MemorySpace.HBM)


def call(body, outs, specs, scratch, name, out_spec=VMEM, flops=100_000_000):
    shapes = []
    for item in outs:
        shape, dtype = item if isinstance(item[0], tuple) else (item, F32)
        shapes.append(jax.ShapeDtypeStruct(shape, dtype))
    return pl.pallas_call(
        body,
        out_shape=tuple(shapes),
        in_specs=specs,
        out_specs=tuple(out_spec for _ in outs),
        scratch_shapes=scratch,
        name=name,
        compiler_params=pltpu.CompilerParams(vmem_limit_bytes=16 << 20),
    )


def shards(nodal_state, inverse_jacobian, speeds, refine_flags, send_index, face_source):
    elements = nodal_state.shape[2]
    groups = elements // LANES
    total = lax.axis_size("curve")
    half = total // 2
    idx = send_index.reshape(-1, LANES)
    jac = inverse_jacobian.reshape(groups, LANES)
    flags = refine_flags.reshape(groups, LANES)
    degrees = np.arange(4)
    top = (np.maximum(np.maximum(degrees[:, None, None], degrees[None, :, None]), degrees) == 3).reshape(64, 1)
    kron = np.kron(MODES, np.kron(MODES, MODES))
    modes = jnp.asarray(np.concatenate([kron, np.repeat(top, 64, axis=1)], axis=1), F32)
    slabs = 5 * groups

    outs = call(
        send_kernel,
        [(88, LANES)] * 4
        + [
            (slabs, 64, LANES),
            (groups, LANES),
            (groups, LANES),
            ((6, elements), jnp.int32),
            (15, 16, LANES),
            (64, LANES),
        ],
        [HBM] * 7,
        [
            pltpu.VMEM((640, elements), BF),
            pltpu.VMEM((20, 64, LANES), F32),
            pltpu.VMEM((4, 16, LANES), jnp.int32),
            pltpu.VMEM(idx.shape, jnp.int32),
            pltpu.VMEM((groups, LANES), jnp.int32),
            pltpu.VMEM(speeds.shape, F32),
            pltpu.SemaphoreType.DMA((slabs + 6,)),
        ],
        "send",
    )(*(in_hbm(x) for x in (nodal_state, idx, jac, flags, face_source, speeds, modes)))
    sends = outs[:4]
    slab, jac, flags, face_source, speeds, modes = outs[4:]
    pair_a = [(i, i + 1) for i in range(0, total, 2)]
    pair_b = [(i, (i + 1) % total) for i in range(1, total, 2)]
    pair_c = [(i, i + 2) for i in range(total) if (i // 2) % 2 == 0]
    pair_d = [(i, (i + 2) % total) for i in range(total) if (i // 2) % 2 == 1]
    received = [swap(x, pairs) for x, pairs in zip(sends, (pair_a, pair_b, pair_c, pair_d))]

    base, outside = call(
        local_kernel,
        [(slabs, 64, LANES), (6 * groups, 80, LANES)],
        [VMEM] * 5,
        [
            pltpu.VMEM((64, elements), F32),
            pltpu.VMEM((2 * groups, 8, LANES), F32),
            pltpu.VMEM((160, elements), BF),
        ],
        "local",
    )(slab, jac, speeds, modes, face_source)
    rows = slabs // 2 * 64
    first, second, counts, meta, cols = call(
        face_kernel,
        [
            (rows, LANES),
            (rows, LANES),
            (half, LANES),
            ((16, 8 * LANES), BF),
            ((2, 8 * LANES, LANES), jnp.int16),
        ],
        [VMEM] * 11,
        [
            pltpu.VMEM((groups, 16, LANES), F32),
            pltpu.VMEM((6 * groups, 80, LANES), F32),
            pltpu.VMEM((160, 4 * LANES), BF),
        ],
        "faces",
    )(base, slab, outside, face_source, jac, speeds, flags, *(received[q] for q in (3, 1, 2, 0)))

    from_a = swap(first, pair_a)
    from_b = swap(second, pair_b[:-1])

    halves = [list(range(half)), list(range(half, total))]
    counts = lax.all_to_all(counts, "curve", 0, 0, axis_index_groups=halves, tiled=True)

    state, new_jac = call(
        refine_kernel,
        [(5, 64, E_NEW), (1, E_NEW)],
        [VMEM] * 7,
        [
            pltpu.VMEM((640, 8 * LANES), BF),
            pltpu.VMEM((40, 64, LANES), F32),
            pltpu.VMEM((8 * 48, 8, LANES), F32),
            pltpu.VMEM((5, 64, E_NEW), F32),
            pltpu.VMEM((1, E_NEW), F32),
            pltpu.SemaphoreType.DMA((6,)),
        ],
        "refine",
        HBM,
    )(from_b, from_a, first, second, counts, meta, cols)
    return state, new_jac.reshape(E_NEW)


def solution(mesh):
    return jax.shard_map(
        shards,
        mesh=mesh,
        in_specs=(
            P(None, None, "curve"),
            P("curve"),
            P(),
            P("curve"),
            P("curve"),
            P(None, "curve"),
        ),
        out_specs=(P(None, None, "curve"), P("curve")),
        check_vma=False,
    )
```
